32 devices in a mesh: gx: 4 (over x, core), gy: 4 (over z), gz: 2 (over y).
Axes of the slice: x: 2, y: 2, z: 4, core: 2. Of those that a mesh axis runs over, the one named last changes fastest.
Arguments:
- amplitudes: bfloat16 [2, 16384, 2048], P(None, ('gx', 'gy', 'gz')), may hold values from -6 to 6
- pauli_x: int32 [200], replicated, may hold values from 0 to 2047, as said below
- pauli_z: int32 [200], replicated, may hold values from 0 to 2047
- pauli_phase: int32 [200], replicated, may hold values from 0 to 3
Outputs:
- density_real: float32 [2048, 2048], P(('gx', 'gy', 'gz'))
- density_imag: float32 [2048, 2048], P(('gx', 'gy', 'gz'))
- expectations: float32 [2, 200], replicated
The draws below stay inside these ranges and needn't reach their ends.
Inputs may be any that keep to these rules, and one draw needn't show every extreme that they name: Bit q of the mask acts on kept qubit q (the bit of weight 2^q of the last index); pauli_x and pauli_z of a term are never both zero.
All inputs are finite; a program needn't handle non-finite values.
Results may differ from the reference program's by a relative error of at most 0.0003.
Values sent between devices are 32-bit elements; how exact they have to be, the bound alone decides.
A program may use at most 192 MiB of HBM per device.

```python
import jax
import jax.numpy as jnp
from jax import lax

QUBITS = 11
R = 2048
COLS_ALL = 16384
TERMS = 200


def pauli_masks(key):
    flips = jax.random.randint(jax.random.fold_in(key, 11), (TERMS,), 0, R).astype(jnp.int32)
    phases = jax.random.randint(jax.random.fold_in(key, 23), (TERMS,), 0, R).astype(jnp.int32)
    both_zero = jnp.logical_and(flips == 0, phases == 0)
    phases = jnp.where(both_zero, jnp.int32(1), phases)
    return (flips, phases)


def draw_pauli_x(key, part):
    return pauli_masks(key)[0]


def draw_pauli_z(key, part):
    return pauli_masks(key)[1]


def with_ends(result, key, low, top_value):
    shape = result.shape
    index_at = [jax.random.randint(jax.random.fold_in(key, axis), (), 0, shape[axis]) for axis in range(len(shape))]
    result = result.at[tuple(index_at)].set(low)
    longest = shape.index(max(shape))
    index_at[longest] = (index_at[longest] + 1) % shape[longest]
    return result.at[tuple(index_at)].set(top_value)


def shard_levels(key, extent, cuts, low, high):
    gain, own = 1.0, jax.random.fold_in(key, 6)
    for position, parts in cuts:
        heights = jnp.exp(jax.random.uniform(jax.random.fold_in(own, position), (parts,), jnp.float32, low / len(cuts), high / len(cuts)))
        gain = gain * jnp.repeat(heights, extent[position] // parts).reshape([-1 if axis == position else 1 for axis in range(len(extent))])
    return gain


def bell_draw(stream_key, extent, width, limit, shards=(), kind=jnp.bfloat16):
    array = width * jax.random.normal(stream_key, extent, jnp.float32)
    if shards:
        array = array * shard_levels(stream_key, extent, shards, -0.22, 0.18)
    return jnp.clip(array, -limit, limit).astype(kind)


def setup_inputs(seed: int = 0) -> dict:
    streams_of = jax.random.split(jax.random.key(seed), 5)
    return {
        "amplitudes": bell_draw(streams_of[0], (2, COLS_ALL, R), 1.0, 6.0, ((1, 32),)),
        "pauli_x": draw_pauli_x(jax.random.fold_in(streams_of[4], 71), 0),
        "pauli_z": draw_pauli_z(jax.random.fold_in(streams_of[4], 71), 0),
        "pauli_phase": with_ends(jax.random.randint(streams_of[3], (TERMS,), 0, 4), jax.random.fold_in(streams_of[3], 1), 0, 3).astype(jnp.int32),
    }


def parity_sign(values, masks):
    anded = jnp.bitwise_and(values, masks)
    counted = jnp.zeros_like(anded)
    for bit_index in range(QUBITS):
        counted = counted + jnp.bitwise_and(jnp.right_shift(anded, bit_index), 1)
    return (1 - 2 * jnp.bitwise_and(counted, 1)).astype(jnp.float32)


def phase_parts(pauli_phase):
    phase_real = jnp.where(pauli_phase == 0, 1.0, jnp.where(pauli_phase == 2, -1.0, 0.0)).astype(jnp.float32)
    phase_imag = jnp.where(pauli_phase == 1, 1.0, jnp.where(pauli_phase == 3, -1.0, 0.0)).astype(jnp.float32)
    return phase_real, phase_imag


def reference(amplitudes, pauli_x, pauli_z, pauli_phase):
    real_part = amplitudes[0].astype(jnp.float32)
    imag_part = amplitudes[1].astype(jnp.float32)
    dims = (((0,), (0,)), ((), ()))
    high = lax.Precision.HIGHEST
    gram_real = lax.dot_general(real_part, real_part, dims, precision=high) + lax.dot_general(imag_part, imag_part, dims, precision=high)
    gram_imag = lax.dot_general(imag_part, real_part, dims, precision=high) - lax.dot_general(real_part, imag_part, dims, precision=high)
    total_cols = amplitudes.shape[1]
    density_real = gram_real / total_cols
    density_imag = gram_imag / total_cols
    row_ids = jnp.arange(R, dtype=jnp.int32)[None, :]
    partner = jnp.bitwise_xor(row_ids, pauli_x[:, None])
    picked_real = jnp.take_along_axis(density_real, partner.T, axis=1).T
    picked_imag = jnp.take_along_axis(density_imag, partner.T, axis=1).T
    signs = parity_sign(row_ids, pauli_z[:, None])
    phase_real, phase_imag = phase_parts(pauli_phase)
    sum_real = jnp.sum(signs * picked_real, axis=1)
    sum_imag = jnp.sum(signs * picked_imag, axis=1)
    expect_real = phase_real * sum_real - phase_imag * sum_imag
    expect_imag = phase_real * sum_imag + phase_imag * sum_real
    return density_real, density_imag, jnp.stack([expect_real, expect_imag], 0)
```

```python
import functools

import jax
import jax.numpy as jnp
from jax import lax
from jax.experimental import pallas as pl
from jax.experimental.pallas import tpu as pltpu
from jax.sharding import PartitionSpec as P

AXES = ("gx", "gy", "gz")
LANES = 128
EARLY = 2
MESH = pl.DeviceIdType.MESH


def log2(value):
    return value.bit_length() - 1


def flat_index(sizes):
    return (lax.axis_index("gx") * sizes[1] + lax.axis_index("gy")) * sizes[2] + lax.axis_index("gz")


def coords(flat, sizes):
    return (flat // (sizes[1] * sizes[2]), (flat // sizes[2]) % sizes[1], flat % sizes[2])


def flip(bit, by):
    return bit + by - 2 * bit * by


def stage_order(sizes):
    zs = log2(sizes[2])
    ys = log2(sizes[1])
    xs = log2(sizes[0])
    rest_x = [zs + ys + t for t in range(xs - 1, 0, -1)]
    rest_y = [zs + t for t in range(ys)]
    rest_z = list(range(zs - 1, -1, -1))
    order = [zs + ys] + rest_x + rest_y[:1] + rest_z + rest_y[1:]
    trade = order.index(rest_z[0]) if rest_x and rest_z else 1
    return order, trade


def parity_sign(masked):
    shift = 16
    while shift >= 1:
        masked = jnp.bitwise_xor(masked, jnp.right_shift(masked, shift))
        shift //= 2
    return (1 - 2 * jnp.bitwise_and(masked, 1)).astype(jnp.float32)


def row_order(sizes, q):
    nbits = log2(sizes[0] * sizes[1] * sizes[2])
    stages, _ = stage_order(sizes)
    lowbits = log2(q)
    return [p for p in stages[2:3] + stages[4:] + stages[1:2] + stages[3:4] if lowbits <= p < nbits]


def early_items(sizes, q, lag):
    nbits = log2(sizes[0] * sizes[1] * sizes[2])
    stages, trade = stage_order(sizes)
    high = row_order(sizes, q)

    def pair_of(v, half):
        by_stage = [(v >> (nbits - 1 - s)) & 1 for s in range(nbits)]
        if half:
            by_stage[1], by_stage[trade] = by_stage[trade], by_stage[1]
        flips = {p: by_stage[s] for s, p in enumerate(stages)}
        w = 0
        for p in high:
            w = 2 * w + 1 - flips[p]
        return w

    out = []
    for v in range((1 << (nbits - 2)) - 1, (1 << (nbits - 3)) - 1, -1):
        waits = []
        for half in range(2):
            waits.append(2 * pair_of(v, half) + 1 + lag)
            waits.append(2 * pair_of(v | (1 << (nbits - 2)), half) + 1 + 2 * lag)
        out.append((max(waits), v))
    return sorted(out, key=lambda item: (item[0], -item[1]))


def gram_kernel(
    sizes, total_cols, early, amp, px, pz, phase, kept, mirrored, expect,
    ext, part, land, turned, came, spread, tally, outbox, inbox, load_sem, send_sem, recv_sem, msend, mrecv, esend, erecv,
):
    n = sizes[0] * sizes[1] * sizes[2]
    nbits = log2(n)
    depth = amp.shape[1]
    order = amp.shape[2]
    own = order // n
    block = max(own, LANES)
    q = block // own
    blocks = order // block
    width = (blocks // 2 + 1) * block
    slabs = part.shape[1]
    chunks = recv_sem.shape[0] // n
    group = slabs // chunks
    me = flat_index(sizes)
    bits = [(me // (1 << p)) % 2 for p in range(nbits)]
    stages, trade = stage_order(sizes)
    half = bits[stages[0]]
    lag = 4

    def loads():
        out = []
        for part_index in range(2):
            rows = pl.ds(part_index * depth, depth)
            out.append(pltpu.make_async_copy(amp.at[part_index], ext.at[rows, pl.ds(0, order)], load_sem.at[2 * part_index]))
            out.append(
                pltpu.make_async_copy(
                    amp.at[part_index, :, pl.ds(0, width - block)],
                    ext.at[rows, pl.ds(order, width - block)],
                    load_sem.at[2 * part_index + 1],
                )
            )
        return out

    for copy in loads():
        copy.start()

    def flips_of(v):
        by_stage = [(v >> (nbits - 1 - s)) & 1 for s in range(nbits)]
        flips = [0] * nbits
        for s, p in enumerate(stages):
            flips[p] = by_stage[s]
        flips[stages[1]] = by_stage[1] * (1 - half) + by_stage[trade] * half
        flips[stages[trade]] = by_stage[trade] * (1 - half) + by_stage[1] * half
        return flips

    def place(flips):
        return sum((1 << p) * flip(bits[p], flips[p]) for p in range(nbits))

    def name(flips):
        return sum((1 << p) * flips[p] for p in range(nbits))

    partner = [place(flips_of(1 << (nbits - 1 - s))) for s in range(nbits)]
    lowbits = log2(q)
    high = row_order(sizes, q)

    def message(where, ident, target, c):
        piece = pl.ds(c * group, group)
        return pltpu.make_async_remote_copy(
            src_ref=part.at[where, piece],
            dst_ref=land.at[ident, piece],
            send_sem=send_sem.at[ident],
            recv_sem=recv_sem.at[ident * chunks + c],
            device_id=coords(target, sizes),
            device_id_type=MESH,
        )

    def whole(where, ident):
        return pltpu.make_async_remote_copy(
            src_ref=part.at[where],
            dst_ref=land.at[ident],
            send_sem=send_sem.at[ident],
            recv_sem=recv_sem.at[ident * chunks],
            device_id=coords(partner[0], sizes),
            device_id_type=MESH,
        )

    def row_block(u):
        flips = [0] * nbits
        flips[stages[0]] = 1 - u % 2
        for j, p in enumerate(high):
            flips[p] = 1 - (u // (1 << (len(high) - j))) % 2
        return flips

    def with_low(flips, g):
        return [(g >> p) & 1 if p < lowbits else flips[p] for p in range(nbits)]

    def summed(where, names, slab, rows):
        total = part[where, slab, rows, :]
        for ident in names:
            total = total + land[ident, slab, rows, :]
        return total

    def second_stage(w, upto):
        for g in range(q):
            flips = with_low(row_block(2 * w + 1), g)
            goes = flips[stages[1]] * (1 - half) + flips[stages[trade]] * half

            @pl.when(goes == 1)
            def _():
                where, ident = place(flips), name(flips)
                whole(where, ident + (1 << stages[0])).wait_recv()
                for slab in range(slabs):
                    for r in range(0, own, 8):
                        rows = pl.ds(r, 8)
                        part[where, slab, rows, :] = summed(where, [ident + (1 << stages[0])], slab, rows)
                for c in range(upto):
                    message(where, ident, partner[1], c).start()

    def later_second(w, c):
        for g in range(q):
            flips = with_low(row_block(2 * w + 1), g)
            goes = flips[stages[1]] * (1 - half) + flips[stages[trade]] * half

            @pl.when(goes == 1)
            def _():
                message(place(flips), name(flips), partner[1], c).start()

    def arrive(v, upto, c, first):
        names = [name(flips_of(v | (1 << (nbits - 1 - t)))) for t in range(upto)]

        def core_to_core():
            whole(0, names[0]).wait_recv()

        if isinstance(first, bool):
            if first:
                core_to_core()
        else:
            pl.when(first)(core_to_core)
        for ident in names[1:]:
            message(0, ident, partner[0], c).wait_recv()
        return names

    def item(v, s, c, first):
        names = arrive(v, s, c, first)
        flips = flips_of(v)
        where = place(flips)
        for g in range(group):
            slab = c * group + g
            for r in range(0, own, 8):
                rows = pl.ds(r, 8)
                part[where, slab, rows, :] = summed(where, names, slab, rows)
        message(where, name(flips), partner[s], c).start()

    terms = px.shape[1]
    mine = me // q
    sub_me = me % q
    base = me * own

    for copy in loads():
        copy.wait()

    row_in = lax.broadcasted_iota(jnp.int32, (block, block), 0)
    lane_in = lax.broadcasted_iota(jnp.int32, (block, block), 1)
    seconds = early_items(sizes, q, lag)

    def compute(u, _):
        @pl.when(u % 2 == 1)
        def _():
            for g in range(q):
                flips = with_low(row_block(u - 1), g)
                whole(place(flips), name(flips)).start()

        @pl.when((u % 2 == 1) & (u >= 1 + lag))
        def _():
            second_stage((u - lag) // 2, early)

        for at in sorted({at for at, _ in seconds if at < blocks}):

            @pl.when(u == at)
            def _():
                for when, v in seconds:
                    if when == at:
                        item(v, 2, 0, True)

        flips = row_block(u)
        first = sum((1 << p) * flip(bits[p], flips[p]) for p in range(lowbits, nbits))
        start = pl.multiple_of(first * own, block)
        lhs = ext[:, pl.ds(start, block)]
        crossed = jnp.concatenate([lhs[depth:], -lhs[:depth]], 0)
        both = jnp.concatenate([lhs, crossed], 1)
        rhs = ext[:, pl.ds(start, width)]
        rows = lax.dot_general(both, rhs, (((0,), (0,)), ((), ())), preferred_element_type=jnp.float32)
        bound = jnp.where(first // q < blocks // 2, 0, -1)
        near = jnp.where(row_in - lane_in <= 0, rows[:block, :block], rows[block:, :block])
        far = jnp.where(row_in - lane_in <= bound, rows[:block, width - block :], rows[block:, width - block :])
        for sub in range(q):
            at = slice(sub * own, (sub + 1) * own)
            more = slice(block + sub * own, block + (sub + 1) * own)
            for k in range(1, slabs):
                cols = slice(k * block, (k + 1) * block)
                part[first + sub, k - 1, :, 0:block] = rows[at, cols]
                part[first + sub, k - 1, :, block : 2 * block] = rows[more, cols]
            part[first + sub, slabs - 1, :, 0:block] = near[at]
            part[first + sub, slabs - 1, :, block : 2 * block] = far[at]
        return 0

    lax.fori_loop(0, blocks, compute, 0)

    for w in range(max(blocks // 2 - lag // 2, 0), blocks // 2):
        second_stage(w, early)
    for at, v in seconds:
        if at >= blocks:
            item(v, 2, 0, True)

    def send_later(c, _):
        for w in range(blocks // 2):
            later_second(w, c)
        return 0

    lax.fori_loop(early, chunks, send_later, 0)

    turn = phase[...]
    paired = parity_sign(jnp.bitwise_and(px[...], pz[...]))
    wanted = jnp.bitwise_xor(px[...], base)
    lane_terms = lax.broadcasted_iota(jnp.int32, (block, terms), 0)
    row = lax.broadcasted_iota(jnp.int32, (own, block), 0)
    lane = lax.broadcasted_iota(jnp.int32, (own, block), 1)
    ids = base + lax.broadcasted_iota(jnp.int32, (own, terms), 0)
    signs = parity_sign(jnp.bitwise_and(ids, pz[...]))
    signs_real = jnp.where(paired > 0, signs, 0.0)
    signs_imag = jnp.where(paired > 0, 0.0, signs)
    spread[...] = jnp.concatenate([signs_real] * 3 + [signs_imag] * 3, 0).astype(jnp.bfloat16)
    tally[...] = jnp.zeros_like(tally)

    def swapped_rows(values):
        for p in range(log2(own)):
            step = 1 << p
            swapped = jnp.where(
                jnp.bitwise_and(lane, step) != 0,
                pltpu.roll(values, step, 1),
                pltpu.roll(values, block - step, 1),
            )
            values = jnp.where(jnp.bitwise_and(row, step) != 0, swapped, values)
        return values

    def in_three(values):
        high_part = values.astype(jnp.bfloat16)
        rest = values - high_part.astype(jnp.float32)
        middle = rest.astype(jnp.bfloat16)
        low = (rest - middle.astype(jnp.float32)).astype(jnp.bfloat16)
        return [high_part, middle, low]

    def pick(real_values, imag_values, k):
        stacked = jnp.concatenate(in_three(swapped_rows(real_values)) + in_three(swapped_rows(imag_values)), 0)
        sums = lax.dot_general(stacked, spread[...], (((0,), (0,)), ((), ())), preferred_element_type=jnp.float32)
        chosen = jnp.where(lane_terms + ((mine + k) % blocks) * block == wanted, sums, 0.0)
        tally[...] = tally[...] + jnp.sum(chosen, axis=0, keepdims=True)

    def mirror(k, sub, source, slot):
        return pltpu.make_async_remote_copy(
            src_ref=turned.at[source, pl.ds(sub * own, own)],
            dst_ref=came.at[slot * q + sub_me],
            send_sem=msend.at[slot * q + sub],
            recv_sem=mrecv.at[slot * q + sub_me],
            device_id=coords(((mine + k) % blocks) * q + sub, sizes),
            device_id_type=MESH,
        )

    def mirror_from(k, sub, slot):
        return pltpu.make_async_remote_copy(
            src_ref=turned.at[0, pl.ds(sub * own, own)],
            dst_ref=came.at[slot * q + sub],
            send_sem=msend.at[slot * q + sub],
            recv_sem=mrecv.at[slot * q + sub],
            device_id=coords(((mine + k) % blocks) * q + sub, sizes),
            device_id_type=MESH,
        )

    local_row = sub_me * own + row
    bound_me = jnp.where(mine < blocks // 2, 0, -1)

    def finish(c):
        names = arrive(0, nbits, c, c == 0)
        for g in range(group):
            slab = c * group + g
            for r in range(0, own, 8):
                rows = pl.ds(r, 8)
                kept[slab, rows, :] = summed(me, names, slab, rows) / total_cols
            turned[slab] = jnp.concatenate([kept[slab, :, :block], kept[slab, :, block:]], 0).T

            @pl.when(slab < slabs - 1)
            def _():
                for sub in range(q):
                    mirror(slab + 1, sub, slab, slab).start()
                pick(kept[slab, :, :block], kept[slab, :, block:], slab + 1)

        @pl.when(c == chunks - 1)
        def _():
            slab = slabs - 1
            for sub in range(q):
                mirror(slabs, sub, slab, slab).start()

                @pl.when(sub != sub_me)
                def _():
                    mirror(0, sub, slab, slabs).start()

                @pl.when(sub == sub_me)
                def _():
                    mirrored[slabs * q + sub] = turned[slab, sub * own : (sub + 1) * own]

            near = kept[slab, :, :block]
            upper = jnp.where(local_row < lane, near, jnp.where(local_row == lane, 0.5 * near, 0.0))
            pick(upper, jnp.where(local_row > lane, near, 0.0), 0)
            far = kept[slab, :, block:]
            holds = local_row - lane <= bound_me
            pick(jnp.where(holds, far, 0.0), jnp.where(holds, 0.0, far), slabs)

    last = nbits - 2

    def step(t, _):
        for s in range(2, nbits):
            c = t - (s - 2)
            if s == 2:
                first, live = False, c < chunks
            else:
                first, live = c == 0, (c >= 0) & (c < chunks)

            @pl.when(live)
            def _():
                for v in range((1 << (nbits - s)) - 1, (1 << (nbits - 1 - s)) - 1, -1):
                    item(v, s, c, first)

        @pl.when((t >= last) & (t - last < chunks))
        def _():
            finish(t - last)

        return 0

    lax.fori_loop(1, chunks + last, step, 0)

    sums = 2.0 * tally[...]
    sum_real = jnp.where(paired > 0, sums, 0.0)
    sum_imag = jnp.where(paired > 0, 0.0, sums)
    phase_real = jnp.where(turn == 0, 1.0, jnp.where(turn == 2, -1.0, 0.0))
    phase_imag = jnp.where(turn == 1, 1.0, jnp.where(turn == 3, -1.0, 0.0))
    total = jnp.concatenate(
        [phase_real * sum_real - phase_imag * sum_imag, phase_real * sum_imag + phase_imag * sum_real], 0
    )
    outbox[...] = total
    inbox[me] = total

    def share(d, to):
        return pltpu.make_async_remote_copy(
            src_ref=outbox,
            dst_ref=inbox.at[to],
            send_sem=esend.at[d],
            recv_sem=erecv.at[to],
            device_id=coords((me + d) % n, sizes),
            device_id_type=MESH,
        )

    def share_out(d, _):
        share(d, me).start()
        return 0

    lax.fori_loop(1, n, share_out, 0)

    for k in range(1, slabs + 1):
        for sub in range(q):
            slot = (k - 1) * q + sub
            mirror_from(k, sub, k - 1).wait()
            mirrored[slot] = came[slot]
    for sub in range(q):

        @pl.when(sub != sub_me)
        def _():
            mirror_from(0, sub, slabs).wait()
            mirrored[slabs * q + sub] = came[slabs * q + sub]

    def drain(ident, _):
        whole(0, ident).wait_send()
        return 0

    lax.fori_loop(1, n, drain, 0)

    def share_in(d, _):
        share(d, (me + d) % n).wait()
        return 0

    lax.fori_loop(1, n, share_in, 0)

    total = inbox[0]
    for j in range(1, n):
        total = total + inbox[j]
    expect[...] = total


def finish_kernel(sizes, kept, mirrored, expected, real, imag, expect):
    n = sizes[0] * sizes[1] * sizes[2]
    own, order = real.shape
    block = max(own, LANES)
    q = block // own
    blocks = order // block
    slabs = kept.shape[0]
    me = flat_index(sizes)
    mine = me // q
    sub_me = me % q

    def columns(k):
        return pl.ds(pl.multiple_of(((mine + k + blocks) % blocks) * block, block), block)

    def turned(slot, side):
        return jnp.concatenate([mirrored[slot * q + sub][:, side * own : (side + 1) * own] for sub in range(q)], 1)

    for k in range(1, slabs):
        real[:, columns(k)] = kept[k - 1, :, :block]
        imag[:, columns(k)] = kept[k - 1, :, block:]
        real[:, columns(-k)] = turned(k - 1, 0)
        imag[:, columns(-k)] = -turned(k - 1, 1)
    row = sub_me * own + lax.broadcasted_iota(jnp.int32, (own, block), 0)
    lane = lax.broadcasted_iota(jnp.int32, (own, block), 1)
    near, other = kept[slabs - 1, :, :block], turned(slabs, 0)
    real[:, columns(0)] = jnp.where(row <= lane, near, other)
    imag[:, columns(0)] = jnp.where(row > lane, near, jnp.where(row < lane, -other, 0.0))
    far, other = kept[slabs - 1, :, block:], turned(slabs - 1, 1)
    holds = row - lane <= jnp.where(mine < blocks // 2, 0, -1)
    real[:, columns(slabs)] = jnp.where(holds, far, other)
    imag[:, columns(slabs)] = jnp.where(holds, -other, far)
    expect[...] = expected[...]


def on_device(sizes, amplitudes, pauli_x, pauli_z, pauli_phase):
    n = sizes[0] * sizes[1] * sizes[2]
    _, depth, order = amplitudes.shape
    own = order // n
    block = max(own, LANES)
    q = block // own
    blocks = order // block
    slabs = blocks // 2
    group = min(slabs, max(1, LANES // (2 * own)))
    chunks = slabs // group
    width = (slabs + 1) * block
    slots = (slabs + 1) * q
    vmem = pl.BlockSpec(memory_space=pltpu.VMEM)
    terms = pauli_x.shape[0]
    kept, mirrored, expect = pl.pallas_call(
        functools.partial(gram_kernel, sizes, float(depth * n), min(EARLY, chunks)),
        out_shape=(
            jax.ShapeDtypeStruct((slabs, own, 2 * block), jnp.float32),
            jax.ShapeDtypeStruct((slots, own, 2 * own), jnp.float32),
            jax.ShapeDtypeStruct((2, terms), jnp.float32),
        ),
        in_specs=[pl.BlockSpec(memory_space=pl.ANY), vmem, vmem, vmem],
        out_specs=(vmem,) * 3,
        scratch_shapes=[
            pltpu.VMEM((2 * depth, order + width - block), jnp.bfloat16),
            pltpu.VMEM((n, slabs, own, 2 * block), jnp.float32),
            pltpu.VMEM((n, slabs, own, 2 * block), jnp.float32),
            pltpu.VMEM((slabs, block, 2 * own), jnp.float32),
            pltpu.VMEM((slots, own, 2 * own), jnp.float32),
            pltpu.VMEM((6 * own, terms), jnp.bfloat16),
            pltpu.VMEM((1, terms), jnp.float32),
            pltpu.VMEM((2, terms), jnp.float32),
            pltpu.VMEM((n, 2, terms), jnp.float32),
            pltpu.SemaphoreType.DMA((4,)),
            pltpu.SemaphoreType.DMA((n,)),
            pltpu.SemaphoreType.DMA((n * chunks,)),
            pltpu.SemaphoreType.DMA((slots,)),
            pltpu.SemaphoreType.DMA((slots,)),
            pltpu.SemaphoreType.DMA((n,)),
            pltpu.SemaphoreType.DMA((n,)),
        ],
        compiler_params=pltpu.CompilerParams(has_side_effects=True, vmem_limit_bytes=60 << 20),
    )(amplitudes, pauli_x[None], pauli_z[None], pauli_phase[None])
    real, imag, expect = pl.pallas_call(
        functools.partial(finish_kernel, sizes),
        out_shape=(
            jax.ShapeDtypeStruct((own, order), jnp.float32),
            jax.ShapeDtypeStruct((own, order), jnp.float32),
            jax.ShapeDtypeStruct((2, terms), jnp.float32),
        ),
        in_specs=[vmem] * 3,
        out_specs=(vmem,) * 3,
    )(kept, mirrored, expect)
    return real, imag, expect


def solution(mesh):
    sizes = tuple(mesh.shape[axis] for axis in AXES)
    return jax.shard_map(
        functools.partial(on_device, sizes),
        mesh=mesh,
        in_specs=(P(None, AXES, None), P(), P(), P()),
        out_specs=(P(AXES, None), P(AXES, None), P()),
        check_vma=False,
    )
```

```python
import functools

import jax
import jax.numpy as jnp
from jax import lax
from jax.experimental import pallas as pl
from jax.experimental.pallas import tpu as pltpu
from jax.sharding import PartitionSpec as P

AXES = ("gx", "gy", "gz")
LANES = 128
EARLY = 2
VMEM_LIMIT = 60 << 20
MESH = pl.DeviceIdType.MESH


def log2(value):
    return value.bit_length() - 1


def flat_index(sizes):
    return (lax.axis_index("gx") * sizes[1] + lax.axis_index("gy")) * sizes[2] + lax.axis_index("gz")


def coords(flat, sizes):
    return (flat // (sizes[1] * sizes[2]), (flat // sizes[2]) % sizes[1], flat % sizes[2])


def flip(bit, by):
    return bit + by - 2 * bit * by


def stage_order(sizes):
    zs = log2(sizes[2])
    ys = log2(sizes[1])
    xs = log2(sizes[0])
    rest_x = [zs + ys + t for t in range(xs - 1, 0, -1)]
    rest_y = [zs + t for t in range(ys)]
    rest_z = list(range(zs - 1, -1, -1))
    order = [zs + ys] + rest_x + rest_y[:1] + rest_z + rest_y[1:]
    trade = order.index(rest_z[0]) if rest_x and rest_z else 1
    return order, trade


def parity_sign(masked):
    shift = 16
    while shift >= 1:
        masked = jnp.bitwise_xor(masked, jnp.right_shift(masked, shift))
        shift //= 2
    return (1 - 2 * jnp.bitwise_and(masked, 1)).astype(jnp.float32)


def row_order(sizes, q):
    nbits = log2(sizes[0] * sizes[1] * sizes[2])
    stages, _ = stage_order(sizes)
    lowbits = log2(q)
    return [p for p in stages[2:3] + stages[4:] + stages[1:2] + stages[3:4] if lowbits <= p < nbits]


def early_items(sizes, q, lag, flight):
    nbits = log2(sizes[0] * sizes[1] * sizes[2])
    stages, trade = stage_order(sizes)
    high = row_order(sizes, q)

    def pair_of(v, half):
        by_stage = [(v >> (nbits - 1 - s)) & 1 for s in range(nbits)]
        if half:
            by_stage[1], by_stage[trade] = by_stage[trade], by_stage[1]
        flips = {p: by_stage[s] for s, p in enumerate(stages)}
        w = 0
        for p in high:
            w = 2 * w + 1 - flips[p]
        return w

    out = []
    for v in range((1 << (nbits - 2)) - 1, (1 << (nbits - 3)) - 1, -1):
        waits = []
        for half in range(2):
            waits.append(2 * pair_of(v, half) + 1 + lag)
            waits.append(2 * pair_of(v | (1 << (nbits - 2)), half) + 1 + lag + flight)
        out.append((max(waits), v))
    return sorted(out, key=lambda item: (item[0], -item[1]))


def gram_kernel(
    sizes, total_cols, early, amp, px, pz, phase, kept, mirrored, expect,
    ext, part, land, turned, came, spread, tally, outbox, inbox, load_sem, send_sem, recv_sem, msend, mrecv, esend, erecv,
):
    n = sizes[0] * sizes[1] * sizes[2]
    nbits = log2(n)
    depth = amp.shape[1]
    order = amp.shape[2]
    own = order // n
    block = max(own, LANES)
    q = block // own
    blocks = order // block
    width = (blocks // 2 + 1) * block
    slabs = part.shape[1]
    chunks = recv_sem.shape[0] // n
    group = slabs // chunks
    passes = 2
    per_pass = chunks // passes
    part_slabs = slabs // passes
    me = flat_index(sizes)
    bits = [(me // (1 << p)) % 2 for p in range(nbits)]
    stages, trade = stage_order(sizes)
    half = bits[stages[0]]
    lag, late_lag, flight = 4, blocks // 2, 6

    def loads():
        out = []
        for part_index in range(2):
            rows = pl.ds(part_index * depth, depth)
            out.append(pltpu.make_async_copy(amp.at[part_index], ext.at[rows, pl.ds(0, order)], load_sem.at[2 * part_index]))
            out.append(
                pltpu.make_async_copy(
                    amp.at[part_index, :, pl.ds(0, width - block)],
                    ext.at[rows, pl.ds(order, width - block)],
                    load_sem.at[2 * part_index + 1],
                )
            )
        return out


    def flips_of(v):
        by_stage = [(v >> (nbits - 1 - s)) & 1 for s in range(nbits)]
        flips = [0] * nbits
        for s, p in enumerate(stages):
            flips[p] = by_stage[s]
        flips[stages[1]] = by_stage[1] * (1 - half) + by_stage[trade] * half
        flips[stages[trade]] = by_stage[trade] * (1 - half) + by_stage[1] * half
        return flips

    def place(flips):
        return sum((1 << p) * flip(bits[p], flips[p]) for p in range(nbits))

    def name(flips):
        return sum((1 << p) * flips[p] for p in range(nbits))

    partner = [place(flips_of(1 << (nbits - 1 - s))) for s in range(nbits)]
    barrier = pltpu.get_barrier_semaphore()
    for other in partner:
        pl.semaphore_signal(barrier, inc=1, device_id=coords(other, sizes), device_id_type=MESH)
    for copy in loads():
        copy.start()
    lowbits = log2(q)
    high = row_order(sizes, q)

    def message(where, ident, target, c):
        piece = pl.ds(c * group, group)
        return pltpu.make_async_remote_copy(
            src_ref=part.at[where, piece],
            dst_ref=land.at[ident, piece],
            send_sem=send_sem.at[ident],
            recv_sem=recv_sem.at[ident * chunks + c],
            device_id=coords(target, sizes),
            device_id_type=MESH,
        )

    def across(where, ident, which):
        piece = pl.ds(which * part_slabs, part_slabs)
        return pltpu.make_async_remote_copy(
            src_ref=part.at[where, piece],
            dst_ref=land.at[ident, piece],
            send_sem=send_sem.at[ident],
            recv_sem=recv_sem.at[ident * chunks + which],
            device_id=coords(partner[0], sizes),
            device_id_type=MESH,
        )

    def row_block(u):
        flips = [0] * nbits
        flips[stages[0]] = 1 - u % 2
        for j, p in enumerate(high):
            flips[p] = 1 - (u // (1 << (len(high) - j))) % 2
        return flips

    def with_low(flips, g):
        return [(g >> p) & 1 if p < lowbits else flips[p] for p in range(nbits)]

    def summed(where, names, slab, rows):
        total = part[where, slab, rows, :]
        for ident in names:
            total = total + land[ident, slab, rows, :]
        return total

    def second_stage(w, which, upto):
        for g in range(q):
            flips = with_low(row_block(2 * w + 1), g)
            goes = flips[stages[1]] * (1 - half) + flips[stages[trade]] * half

            @pl.when(goes == 1)
            def _():
                where, ident = place(flips), name(flips)
                across(where, ident + (1 << stages[0]), which).wait_recv()
                for slab in range(which * part_slabs, (which + 1) * part_slabs):
                    for r in range(0, own, 8):
                        rows = pl.ds(r, 8)
                        part[where, slab, rows, :] = summed(where, [ident + (1 << stages[0])], slab, rows)
                for c in range(which * per_pass, which * per_pass + upto):
                    message(where, ident, partner[1], c).start()

    def later_second(w, c):
        for g in range(q):
            flips = with_low(row_block(2 * w + 1), g)
            goes = flips[stages[1]] * (1 - half) + flips[stages[trade]] * half

            @pl.when(goes == 1)
            def _():
                message(place(flips), name(flips), partner[1], c).start()

    def arrive(v, upto, c):
        names = [name(flips_of(v | (1 << (nbits - 1 - t)))) for t in range(upto)]

        @pl.when(c % per_pass == 0)
        def _():
            across(0, names[0], c // per_pass).wait_recv()

        for ident in names[1:]:
            message(0, ident, partner[0], c).wait_recv()
        return names

    def item(v, s, c):
        names = arrive(v, s, c)
        flips = flips_of(v)
        where = place(flips)
        for g in range(group):
            slab = c * group + g
            for r in range(0, own, 8):
                rows = pl.ds(r, 8)
                part[where, slab, rows, :] = summed(where, names, slab, rows)
        message(where, name(flips), partner[s], c).start()

    terms = px.shape[1]
    mine = me // q
    sub_me = me % q
    base = me * own

    for copy in loads():
        copy.wait()

    row_in = lax.broadcasted_iota(jnp.int32, (block, block), 0)
    lane_in = lax.broadcasted_iota(jnp.int32, (block, block), 1)
    seconds = early_items(sizes, q, lag, flight)

    def gram(u, which):
        flips = row_block(u)
        first = sum((1 << p) * flip(bits[p], flips[p]) for p in range(lowbits, nbits))
        start = pl.multiple_of(first * own, block)
        lhs = ext[:, pl.ds(start, block)]
        crossed = jnp.concatenate([lhs[depth:], -lhs[:depth]], 0)
        both = jnp.concatenate([lhs, crossed], 1)

        def product(k, count):
            rhs = ext[:, pl.ds(pl.multiple_of(start + k * block, block), count * block)]
            return lax.dot_general(both, rhs, (((0,), (0,)), ((), ())), preferred_element_type=jnp.float32)

        low = which * part_slabs
        rows = product(low + 1, part_slabs)
        closing = which == passes - 1
        plain = part_slabs - 1 if closing else part_slabs
        if closing:
            here = product(0, 1)
            far_cols = slice(plain * block, (plain + 1) * block)
            bound = jnp.where(first // q < blocks // 2, 0, -1)
            near = jnp.where(row_in - lane_in <= 0, here[:block], here[block:])
            far = jnp.where(row_in - lane_in <= bound, rows[:block, far_cols], rows[block:, far_cols])
        for sub in range(q):
            at = slice(sub * own, (sub + 1) * own)
            more = slice(block + sub * own, block + (sub + 1) * own)
            for k in range(plain):
                cols = slice(k * block, (k + 1) * block)
                part[first + sub, low + k, :, 0:block] = rows[at, cols]
                part[first + sub, low + k, :, block : 2 * block] = rows[more, cols]
            if closing:
                part[first + sub, slabs - 1, :, 0:block] = near[at]
                part[first + sub, slabs - 1, :, block : 2 * block] = far[at]

    def hand_over(u, which):
        for g in range(q):
            flips = with_low(row_block(u), g)
            across(place(flips), name(flips), which).start()

    def compute(u, _):
        @pl.when(u == 1)
        def _():
            pl.semaphore_wait(barrier, nbits)

        @pl.when(u % 2 == 1)
        def _():
            hand_over(u - 1, 0)

        @pl.when((u % 2 == 1) & (u >= 1 + lag))
        def _():
            second_stage((u - lag) // 2, 0, early)

        for at in sorted({at for at, _ in seconds if at < blocks}):

            @pl.when(u == at)
            def _():
                for when, v in seconds:
                    if when == at:
                        item(v, 2, 0)

        gram(u, 0)
        return 0

    def compute_late(u, _):
        @pl.when(u % 2 == 1)
        def _():
            hand_over(u - 1, 1)

        @pl.when((u % 2 == 1) & (u >= 1 + late_lag))
        def _():
            second_stage((u - late_lag) // 2, 1, 1)

        gram(u, 1)
        return 0

    def send_later(c):
        for w in range(blocks // 2):
            later_second(w, c)

    lax.fori_loop(0, blocks, compute, 0)

    for w in range(max(blocks // 2 - lag // 2, 0), blocks // 2):
        second_stage(w, 0, early)
    for at, v in seconds:
        if at >= blocks:
            item(v, 2, 0)
    for c in range(early, per_pass):
        send_later(c)

    inside = per_pass >= 4
    if not inside:
        lax.fori_loop(0, blocks, compute_late, 0)
        for w in range(max(blocks // 2 - late_lag // 2, 0), blocks // 2):
            second_stage(w, 1, per_pass)

    turn = phase[...]
    paired = parity_sign(jnp.bitwise_and(px[...], pz[...]))
    wanted = jnp.bitwise_xor(px[...], base)
    lane_terms = lax.broadcasted_iota(jnp.int32, (block, terms), 0)
    row = lax.broadcasted_iota(jnp.int32, (own, block), 0)
    lane = lax.broadcasted_iota(jnp.int32, (own, block), 1)
    ids = base + lax.broadcasted_iota(jnp.int32, (own, terms), 0)
    signs = parity_sign(jnp.bitwise_and(ids, pz[...]))
    signs_real = jnp.where(paired > 0, signs, 0.0)
    signs_imag = jnp.where(paired > 0, 0.0, signs)
    spread[...] = jnp.concatenate([signs_real] * 3 + [signs_imag] * 3, 0).astype(jnp.bfloat16)
    tally[...] = jnp.zeros_like(tally)

    def swapped_rows(values):
        for p in range(log2(own)):
            step = 1 << p
            swapped = jnp.where(
                jnp.bitwise_and(lane, step) != 0,
                pltpu.roll(values, step, 1),
                pltpu.roll(values, block - step, 1),
            )
            values = jnp.where(jnp.bitwise_and(row, step) != 0, swapped, values)
        return values

    def in_three(values):
        high_part = values.astype(jnp.bfloat16)
        rest = values - high_part.astype(jnp.float32)
        middle = rest.astype(jnp.bfloat16)
        low = (rest - middle.astype(jnp.float32)).astype(jnp.bfloat16)
        return [high_part, middle, low]

    def pick(real_values, imag_values, k):
        stacked = jnp.concatenate(in_three(swapped_rows(real_values)) + in_three(swapped_rows(imag_values)), 0)
        sums = lax.dot_general(stacked, spread[...], (((0,), (0,)), ((), ())), preferred_element_type=jnp.float32)
        chosen = jnp.where(lane_terms + ((mine + k) % blocks) * block == wanted, sums, 0.0)
        tally[...] = tally[...] + jnp.sum(chosen, axis=0, keepdims=True)

    def mirror(k, sub, source, slot):
        return pltpu.make_async_remote_copy(
            src_ref=turned.at[source, pl.ds(sub * own, own)],
            dst_ref=came.at[slot * q + sub_me],
            send_sem=msend.at[slot * q + sub],
            recv_sem=mrecv.at[slot * q + sub_me],
            device_id=coords(((mine + k) % blocks) * q + sub, sizes),
            device_id_type=MESH,
        )

    def mirror_from(k, sub, slot):
        return pltpu.make_async_remote_copy(
            src_ref=turned.at[0, pl.ds(sub * own, own)],
            dst_ref=came.at[slot * q + sub],
            send_sem=msend.at[slot * q + sub],
            recv_sem=mrecv.at[slot * q + sub],
            device_id=coords(((mine + k) % blocks) * q + sub, sizes),
            device_id_type=MESH,
        )

    local_row = sub_me * own + row
    bound_me = jnp.where(mine < blocks // 2, 0, -1)

    def finish(c):
        names = arrive(0, nbits, c)
        for g in range(group):
            slab = c * group + g
            for r in range(0, own, 8):
                rows = pl.ds(r, 8)
                kept[slab, rows, :] = summed(me, names, slab, rows) / total_cols
            turned[slab] = jnp.concatenate([kept[slab, :, :block], kept[slab, :, block:]], 0).T

            @pl.when(slab < slabs - 1)
            def _():
                for sub in range(q):
                    mirror(slab + 1, sub, slab, slab).start()
                pick(kept[slab, :, :block], kept[slab, :, block:], slab + 1)

        @pl.when(c == chunks - 1)
        def _():
            slab = slabs - 1
            for sub in range(q):
                mirror(slabs, sub, slab, slab).start()

                @pl.when(sub != sub_me)
                def _():
                    mirror(0, sub, slab, slabs).start()

                @pl.when(sub == sub_me)
                def _():
                    mirrored[slabs * q + sub] = turned[slab, sub * own : (sub + 1) * own]

            near = kept[slab, :, :block]
            upper = jnp.where(local_row < lane, near, jnp.where(local_row == lane, 0.5 * near, 0.0))
            pick(upper, jnp.where(local_row > lane, near, 0.0), 0)
            far = kept[slab, :, block:]
            holds = local_row - lane <= bound_me
            pick(jnp.where(holds, far, 0.0), jnp.where(holds, 0.0, far), slabs)

    last = nbits - 2

    def step(t, _):
        for s in range(2, nbits):
            c = t - (s - 2)

            @pl.when((c >= 0) & (c < chunks))
            def _():
                for v in range((1 << (nbits - s)) - 1, (1 << (nbits - 1 - s)) - 1, -1):
                    item(v, s, c)

            if s == 2 and inside:

                @pl.when(t < 3)
                def _():
                    lax.fori_loop((t - 1) * (blocks // 2), t * (blocks // 2), compute_late, 0)

                @pl.when(t == 3)
                def _():
                    for w in range(blocks // 2 - late_lag // 2, blocks // 2):
                        second_stage(w, 1, 1)

                @pl.when((t >= 3) & (t - 3 < per_pass - 1))
                def _():
                    send_later(per_pass + t - 2)

        @pl.when((t >= last) & (t - last < chunks))
        def _():
            finish(t - last)

        return 0

    lax.fori_loop(1, chunks + last, step, 0)

    sums = 2.0 * tally[...]
    sum_real = jnp.where(paired > 0, sums, 0.0)
    sum_imag = jnp.where(paired > 0, 0.0, sums)
    phase_real = jnp.where(turn == 0, 1.0, jnp.where(turn == 2, -1.0, 0.0))
    phase_imag = jnp.where(turn == 1, 1.0, jnp.where(turn == 3, -1.0, 0.0))
    total = jnp.concatenate(
        [phase_real * sum_real - phase_imag * sum_imag, phase_real * sum_imag + phase_imag * sum_real], 0
    )
    outbox[...] = total
    inbox[me] = total

    def share(d, to):
        return pltpu.make_async_remote_copy(
            src_ref=outbox,
            dst_ref=inbox.at[to],
            send_sem=esend.at[d],
            recv_sem=erecv.at[to],
            device_id=coords((me + d) % n, sizes),
            device_id_type=MESH,
        )

    def share_out(d, _):
        share(d, me).start()
        return 0

    lax.fori_loop(1, n, share_out, 0)

    for k in range(1, slabs + 1):
        for sub in range(q):
            slot = (k - 1) * q + sub
            mirror_from(k, sub, k - 1).wait()
            mirrored[slot] = came[slot]
    for sub in range(q):

        @pl.when(sub != sub_me)
        def _():
            mirror_from(0, sub, slabs).wait()
            mirrored[slabs * q + sub] = came[slabs * q + sub]

    def drain(ident, _):
        pltpu.make_async_remote_copy(
            src_ref=part.at[0],
            dst_ref=land.at[ident],
            send_sem=send_sem.at[ident],
            recv_sem=recv_sem.at[0],
            device_id=coords(partner[0], sizes),
            device_id_type=MESH,
        ).wait_send()
        return 0

    lax.fori_loop(1, n, drain, 0)

    def share_in(d, _):
        share(d, (me + d) % n).wait()
        return 0

    lax.fori_loop(1, n, share_in, 0)

    total = inbox[0]
    for j in range(1, n):
        total = total + inbox[j]
    expect[...] = total


def finish_kernel(sizes, kept, mirrored, expected, real, imag, expect):
    n = sizes[0] * sizes[1] * sizes[2]
    own, order = real.shape
    block = max(own, LANES)
    q = block // own
    blocks = order // block
    slabs = kept.shape[0]
    me = flat_index(sizes)
    mine = me // q
    sub_me = me % q

    def columns(k):
        return pl.ds(pl.multiple_of(((mine + k + blocks) % blocks) * block, block), block)

    def turned(slot, side):
        return jnp.concatenate([mirrored[slot * q + sub][:, side * own : (side + 1) * own] for sub in range(q)], 1)

    for k in range(1, slabs):
        real[:, columns(k)] = kept[k - 1, :, :block]
        imag[:, columns(k)] = kept[k - 1, :, block:]
        real[:, columns(-k)] = turned(k - 1, 0)
        imag[:, columns(-k)] = -turned(k - 1, 1)
    row = sub_me * own + lax.broadcasted_iota(jnp.int32, (own, block), 0)
    lane = lax.broadcasted_iota(jnp.int32, (own, block), 1)
    near, other = kept[slabs - 1, :, :block], turned(slabs, 0)
    real[:, columns(0)] = jnp.where(row <= lane, near, other)
    imag[:, columns(0)] = jnp.where(row > lane, near, jnp.where(row < lane, -other, 0.0))
    far, other = kept[slabs - 1, :, block:], turned(slabs - 1, 1)
    holds = row - lane <= jnp.where(mine < blocks // 2, 0, -1)
    real[:, columns(slabs)] = jnp.where(holds, far, other)
    imag[:, columns(slabs)] = jnp.where(holds, -other, far)
    expect[...] = expected[...]


def on_device(sizes, amplitudes, pauli_x, pauli_z, pauli_phase):
    n = sizes[0] * sizes[1] * sizes[2]
    _, depth, order = amplitudes.shape
    own = order // n
    block = max(own, LANES)
    q = block // own
    blocks = order // block
    slabs = blocks // 2
    group = min(slabs, max(1, LANES // (2 * own)))
    chunks = slabs // group
    width = (slabs + 1) * block
    slots = (slabs + 1) * q
    vmem = pl.BlockSpec(memory_space=pltpu.VMEM)
    terms = pauli_x.shape[0]
    kept, mirrored, expect = pl.pallas_call(
        functools.partial(gram_kernel, sizes, float(depth * n), min(EARLY, chunks // 2)),
        out_shape=(
            jax.ShapeDtypeStruct((slabs, own, 2 * block), jnp.float32),
            jax.ShapeDtypeStruct((slots, own, 2 * own), jnp.float32),
            jax.ShapeDtypeStruct((2, terms), jnp.float32),
        ),
        in_specs=[pl.BlockSpec(memory_space=pl.ANY), vmem, vmem, vmem],
        out_specs=(vmem,) * 3,
        scratch_shapes=[
            pltpu.VMEM((2 * depth, order + width - block), jnp.bfloat16),
            pltpu.VMEM((n, slabs, own, 2 * block), jnp.float32),
            pltpu.VMEM((n, slabs, own, 2 * block), jnp.float32),
            pltpu.VMEM((slabs, block, 2 * own), jnp.float32),
            pltpu.VMEM((slots, own, 2 * own), jnp.float32),
            pltpu.VMEM((6 * own, terms), jnp.bfloat16),
            pltpu.VMEM((1, terms), jnp.float32),
            pltpu.VMEM((2, terms), jnp.float32),
            pltpu.VMEM((n, 2, terms), jnp.float32),
            pltpu.SemaphoreType.DMA((4,)),
            pltpu.SemaphoreType.DMA((n,)),
            pltpu.SemaphoreType.DMA((n * chunks,)),
            pltpu.SemaphoreType.DMA((slots,)),
            pltpu.SemaphoreType.DMA((slots,)),
            pltpu.SemaphoreType.DMA((n,)),
            pltpu.SemaphoreType.DMA((n,)),
        ],
        compiler_params=pltpu.CompilerParams(collective_id=0, has_side_effects=True, vmem_limit_bytes=VMEM_LIMIT),
    )(amplitudes, pauli_x[None], pauli_z[None], pauli_phase[None])
    real, imag, expect = pl.pallas_call(
        functools.partial(finish_kernel, sizes),
        out_shape=(
            jax.ShapeDtypeStruct((own, order), jnp.float32),
            jax.ShapeDtypeStruct((own, order), jnp.float32),
            jax.ShapeDtypeStruct((2, terms), jnp.float32),
        ),
        in_specs=[vmem] * 3,
        out_specs=(vmem,) * 3,
    )(kept, mirrored, expect)
    return real, imag, expect


def solution(mesh):
    sizes = tuple(mesh.shape[axis] for axis in AXES)
    return jax.shard_map(
        functools.partial(on_device, sizes),
        mesh=mesh,
        in_specs=(P(None, AXES, None), P(), P(), P()),
        out_specs=(P(AXES, None), P(AXES, None), P()),
        check_vma=False,
    )
```

```python
import functools

import jax
import jax.numpy as jnp
from jax import lax
from jax.experimental import pallas as pl
from jax.experimental.pallas import tpu as pltpu
from jax.sharding import PartitionSpec as P

AXES = ("gx", "gy", "gz")
LANES = 128
EARLY = 2
OFFSETS = (0.0, 0.246, 0.02)
SPREAD = 0.4
FINISH_AT = 0.124
REFLECT_AFTER = 0.145
GRAMS_AT = (0.5, 0.75, 0.8)
VMEM_LIMIT = 60 << 20
MESH = pl.DeviceIdType.MESH


def log2(value):
    return value.bit_length() - 1


def flat_index(sizes):
    return (lax.axis_index("gx") * sizes[1] + lax.axis_index("gy")) * sizes[2] + lax.axis_index("gz")


def coords(flat, sizes):
    return (flat // (sizes[1] * sizes[2]), (flat // sizes[2]) % sizes[1], flat % sizes[2])


def flip(bit, by):
    return bit + by - 2 * bit * by


def stage_order(sizes):
    zs = log2(sizes[2])
    ys = log2(sizes[1])
    xs = log2(sizes[0])
    rest_x = [zs + ys + t for t in range(xs - 1, 0, -1)]
    rest_y = [zs + t for t in range(ys)]
    rest_z = list(range(zs - 1, -1, -1))
    order = [zs + ys] + rest_x + rest_y[:1] + rest_z + rest_y[1:]
    trade = order.index(rest_z[0]) if rest_x and rest_z else 1
    return order, trade


def parity_sign(masked):
    shift = 16
    while shift >= 1:
        masked = jnp.bitwise_xor(masked, jnp.right_shift(masked, shift))
        shift //= 2
    return (1 - 2 * jnp.bitwise_and(masked, 1)).astype(jnp.float32)


def row_order(sizes, q):
    nbits = log2(sizes[0] * sizes[1] * sizes[2])
    stages, _ = stage_order(sizes)
    lowbits = log2(q)
    return [p for p in stages[2:3] + stages[4:] + stages[1:2] + stages[3:4] if lowbits <= p < nbits]


def early_items(sizes, q, lag, flight):
    nbits = log2(sizes[0] * sizes[1] * sizes[2])
    stages, trade = stage_order(sizes)
    high = row_order(sizes, q)

    def pair_of(v, half):
        by_stage = [(v >> (nbits - 1 - s)) & 1 for s in range(nbits)]
        if half:
            by_stage[1], by_stage[trade] = by_stage[trade], by_stage[1]
        flips = {p: by_stage[s] for s, p in enumerate(stages)}
        w = 0
        for p in high:
            w = 2 * w + 1 - flips[p]
        return w

    out = []
    for v in range((1 << (nbits - 2)) - 1, (1 << (nbits - 3)) - 1, -1):
        waits = []
        for half in range(2):
            waits.append(2 * pair_of(v, half) + 1 + lag)
            waits.append(2 * pair_of(v | (1 << (nbits - 2)), half) + 1 + lag + flight)
        out.append((max(waits), v))
    return sorted(out, key=lambda item: (item[0], -item[1]))


def gram_kernel(
    sizes, total_cols, early, amp, px, pz, phase, kept, mirrored, expect,
    ext, part, land, turned, came, spread, tally, outbox, inbox, load_sem, send_sem, recv_sem, msend, mrecv, esend, erecv,
):
    n = sizes[0] * sizes[1] * sizes[2]
    nbits = log2(n)
    depth = amp.shape[1]
    order = amp.shape[2]
    own = order // n
    block = max(own, LANES)
    q = block // own
    blocks = order // block
    width = (blocks // 2 + 1) * block
    slabs = part.shape[1]
    chunks = recv_sem.shape[0] // n
    group = slabs // chunks
    passes = 2
    per_pass = chunks // passes
    part_slabs = slabs // passes
    me = flat_index(sizes)
    bits = [(me // (1 << p)) % 2 for p in range(nbits)]
    stages, trade = stage_order(sizes)
    half = bits[stages[0]]
    lag, late_lag, flight = 4, blocks // 2, 6

    def loads():
        out = []
        for part_index in range(2):
            rows = pl.ds(part_index * depth, depth)
            out.append(pltpu.make_async_copy(amp.at[part_index], ext.at[rows, pl.ds(0, order)], load_sem.at[2 * part_index]))
            out.append(
                pltpu.make_async_copy(
                    amp.at[part_index, :, pl.ds(0, width - block)],
                    ext.at[rows, pl.ds(order, width - block)],
                    load_sem.at[2 * part_index + 1],
                )
            )
        return out


    def flips_of(v):
        by_stage = [(v >> (nbits - 1 - s)) & 1 for s in range(nbits)]
        flips = [0] * nbits
        for s, p in enumerate(stages):
            flips[p] = by_stage[s]
        flips[stages[1]] = by_stage[1] * (1 - half) + by_stage[trade] * half
        flips[stages[trade]] = by_stage[trade] * (1 - half) + by_stage[1] * half
        return flips

    def place(flips):
        return sum((1 << p) * flip(bits[p], flips[p]) for p in range(nbits))

    def name(flips):
        return sum((1 << p) * flips[p] for p in range(nbits))

    partner = [place(flips_of(1 << (nbits - 1 - s))) for s in range(nbits)]
    barrier = pltpu.get_barrier_semaphore()
    for other in partner:
        pl.semaphore_signal(barrier, inc=1, device_id=coords(other, sizes), device_id_type=MESH)
    for copy in loads():
        copy.start()
    lowbits = log2(q)
    high = row_order(sizes, q)

    def message(where, ident, target, c):
        piece = pl.ds(c * group, group)
        return pltpu.make_async_remote_copy(
            src_ref=part.at[where, piece],
            dst_ref=land.at[ident, piece],
            send_sem=send_sem.at[ident],
            recv_sem=recv_sem.at[ident * chunks + c],
            device_id=coords(target, sizes),
            device_id_type=MESH,
        )

    def across(where, ident, which):
        piece = pl.ds(which * part_slabs, part_slabs)
        return pltpu.make_async_remote_copy(
            src_ref=part.at[where, piece],
            dst_ref=land.at[ident, piece],
            send_sem=send_sem.at[ident],
            recv_sem=recv_sem.at[ident * chunks + which],
            device_id=coords(partner[0], sizes),
            device_id_type=MESH,
        )

    def row_block(u):
        flips = [0] * nbits
        flips[stages[0]] = 1 - u % 2
        for j, p in enumerate(high):
            flips[p] = 1 - (u // (1 << (len(high) - j))) % 2
        return flips

    def with_low(flips, g):
        return [(g >> p) & 1 if p < lowbits else flips[p] for p in range(nbits)]

    def summed(where, names, slab, rows):
        total = part[where, slab, rows, :]
        for ident in names:
            total = total + land[ident, slab, rows, :]
        return total

    def join(w, which, upto):
        for g in range(q):
            flips = with_low(row_block(2 * w + 1), g)
            where, ident = place(flips), name(flips)
            across(where, ident + (1 << stages[0]), which).wait_recv()
            for slab in range(which * part_slabs, (which + 1) * part_slabs):
                for r in range(0, own, 8):
                    rows = pl.ds(r, 8)
                    part[where, slab, rows, :] = summed(where, [ident + (1 << stages[0])], slab, rows)
        for c in range(which * per_pass, which * per_pass + upto):
            send_first(w, c)

    def send_first(w, c):
        for g in range(q):
            flips = with_low(row_block(2 * w + 1), g)
            goes = flips[stages[1]] * (1 - half) + flips[stages[trade]] * half

            @pl.when(goes == 1)
            def _():
                message(place(flips), name(flips), partner[1], c).start()

    def arrive(v, upto, c):
        names = [name(flips_of(v | (1 << (nbits - 1 - t)))) for t in range(1, upto)]
        for ident in names:
            message(0, ident, partner[0], c).wait_recv()
        return names

    def item(v, s, c):
        names = arrive(v, s, c)
        flips = flips_of(v)
        where = place(flips)
        for g in range(group):
            slab = c * group + g
            for r in range(0, own, 8):
                rows = pl.ds(r, 8)
                part[where, slab, rows, :] = summed(where, names, slab, rows)
        message(where, name(flips), partner[s], c).start()

    terms = px.shape[1]
    mine = me // q
    sub_me = me % q
    base = me * own

    for copy in loads():
        copy.wait()

    row_in = lax.broadcasted_iota(jnp.int32, (block, block), 0)
    lane_in = lax.broadcasted_iota(jnp.int32, (block, block), 1)
    seconds = early_items(sizes, q, lag, flight)

    def gram(u, which):
        flips = row_block(u)
        first = sum((1 << p) * flip(bits[p], flips[p]) for p in range(lowbits, nbits))
        start = pl.multiple_of(first * own, block)
        lhs = ext[:, pl.ds(start, block)]
        crossed = jnp.concatenate([lhs[depth:], -lhs[:depth]], 0)
        both = jnp.concatenate([lhs, crossed], 1)

        def product(k, count):
            rhs = ext[:, pl.ds(pl.multiple_of(start + k * block, block), count * block)]
            return lax.dot_general(both, rhs, (((0,), (0,)), ((), ())), preferred_element_type=jnp.float32)

        low = which * part_slabs
        rows = product(low + 1, part_slabs)
        closing = which == passes - 1
        plain = part_slabs - 1 if closing else part_slabs
        if closing:
            here = product(0, 1)
            far_cols = slice(plain * block, (plain + 1) * block)
            bound = jnp.where(first // q < blocks // 2, 0, -1)
            near = jnp.where(row_in - lane_in <= 0, here[:block], here[block:])
            far = jnp.where(row_in - lane_in <= bound, rows[:block, far_cols], rows[block:, far_cols])
        for sub in range(q):
            at = slice(sub * own, (sub + 1) * own)
            more = slice(block + sub * own, block + (sub + 1) * own)
            for k in range(plain):
                cols = slice(k * block, (k + 1) * block)
                part[first + sub, low + k, :, 0:block] = rows[at, cols]
                part[first + sub, low + k, :, block : 2 * block] = rows[more, cols]
            if closing:
                part[first + sub, slabs - 1, :, 0:block] = near[at]
                part[first + sub, slabs - 1, :, block : 2 * block] = far[at]

    def hand_over(u, which):
        for g in range(q):
            flips = with_low(row_block(u), g)
            across(place(flips), name(flips), which).start()

    def compute(u, _):
        @pl.when(u == 1)
        def _():
            pl.semaphore_wait(barrier, nbits)

        @pl.when(u % 2 == 1)
        def _():
            hand_over(u - 1, 0)

        @pl.when((u % 2 == 1) & (u >= 1 + lag))
        def _():
            join((u - lag) // 2, 0, early)

        for at in sorted({at for at, _ in seconds if at < blocks}):

            @pl.when(u == at)
            def _():
                for when, v in seconds:
                    if when == at:
                        item(v, 2, 0)

        gram(u, 0)
        return 0

    def compute_late(u, _):
        @pl.when(u % 2 == 1)
        def _():
            hand_over(u - 1, 1)

        @pl.when((u % 2 == 1) & (u >= 1 + late_lag))
        def _():
            join((u - late_lag) // 2, 1, 1)

        gram(u, 1)
        return 0

    def send_later(c):
        for w in range(blocks // 2):
            send_first(w, c)

    lax.fori_loop(0, blocks, compute, 0)

    for w in range(max(blocks // 2 - lag // 2, 0), blocks // 2):
        join(w, 0, early)
    for at, v in seconds:
        if at >= blocks:
            item(v, 2, 0)
    for c in range(early, per_pass):
        send_later(c)

    inside = per_pass >= 4
    if not inside:
        lax.fori_loop(0, blocks, compute_late, 0)
        for w in range(max(blocks // 2 - late_lag // 2, 0), blocks // 2):
            join(w, 1, per_pass)

    turn = phase[...]
    paired = parity_sign(jnp.bitwise_and(px[...], pz[...]))
    wanted = jnp.bitwise_xor(px[...], base)
    lane_terms = lax.broadcasted_iota(jnp.int32, (block, terms), 0)
    row = lax.broadcasted_iota(jnp.int32, (own, block), 0)
    lane = lax.broadcasted_iota(jnp.int32, (own, block), 1)
    ids = base + lax.broadcasted_iota(jnp.int32, (own, terms), 0)
    signs = parity_sign(jnp.bitwise_and(ids, pz[...]))
    signs_real = jnp.where(paired > 0, signs, 0.0)
    signs_imag = jnp.where(paired > 0, 0.0, signs)
    spread[...] = jnp.concatenate([signs_real] * 3 + [signs_imag] * 3, 0).astype(jnp.bfloat16)
    tally[...] = jnp.zeros_like(tally)

    def swapped_rows(values):
        for p in range(log2(own)):
            step = 1 << p
            swapped = jnp.where(
                jnp.bitwise_and(lane, step) != 0,
                pltpu.roll(values, step, 1),
                pltpu.roll(values, block - step, 1),
            )
            values = jnp.where(jnp.bitwise_and(row, step) != 0, swapped, values)
        return values

    def in_three(values):
        high_part = values.astype(jnp.bfloat16)
        rest = values - high_part.astype(jnp.float32)
        middle = rest.astype(jnp.bfloat16)
        low = (rest - middle.astype(jnp.float32)).astype(jnp.bfloat16)
        return [high_part, middle, low]

    def pick(real_values, imag_values, k):
        stacked = jnp.concatenate(in_three(swapped_rows(real_values)) + in_three(swapped_rows(imag_values)), 0)
        sums = lax.dot_general(stacked, spread[...], (((0,), (0,)), ((), ())), preferred_element_type=jnp.float32)
        chosen = jnp.where(lane_terms + ((mine + k) % blocks) * block == wanted, sums, 0.0)
        tally[...] = tally[...] + jnp.sum(chosen, axis=0, keepdims=True)

    def mirror(k, sub, source, slot):
        return pltpu.make_async_remote_copy(
            src_ref=turned.at[source, pl.ds(sub * own, own)],
            dst_ref=came.at[slot * q + sub_me],
            send_sem=msend.at[slot * q + sub],
            recv_sem=mrecv.at[slot * q + sub_me],
            device_id=coords(((mine + k) % blocks) * q + sub, sizes),
            device_id_type=MESH,
        )

    def mirror_from(k, sub, slot):
        return pltpu.make_async_remote_copy(
            src_ref=turned.at[0, pl.ds(sub * own, own)],
            dst_ref=came.at[slot * q + sub],
            send_sem=msend.at[slot * q + sub],
            recv_sem=mrecv.at[slot * q + sub],
            device_id=coords(((mine + k) % blocks) * q + sub, sizes),
            device_id_type=MESH,
        )

    local_row = sub_me * own + row
    bound_me = jnp.where(mine < blocks // 2, 0, -1)

    def finish(c):
        names = arrive(0, nbits, c)
        for g in range(group):
            slab = c * group + g
            for r in range(0, own, 8):
                rows = pl.ds(r, 8)
                kept[slab, rows, :] = summed(me, names, slab, rows) / total_cols
            turned[slab] = jnp.concatenate([kept[slab, :, :block], kept[slab, :, block:]], 0).T

            @pl.when(slab < slabs - 1)
            def _():
                pick(kept[slab, :, :block], kept[slab, :, block:], slab + 1)

        @pl.when(c == chunks - 1)
        def _():
            slab = slabs - 1
            near = kept[slab, :, :block]
            upper = jnp.where(local_row < lane, near, jnp.where(local_row == lane, 0.5 * near, 0.0))
            pick(upper, jnp.where(local_row > lane, near, 0.0), 0)
            far = kept[slab, :, block:]
            holds = local_row - lane <= bound_me
            pick(jnp.where(holds, far, 0.0), jnp.where(holds, 0.0, far), slabs)

    def reflect(c):
        for g in range(group):
            slab = c * group + g
            for sub in range(q):
                mirror(slab + 1, sub, slab, slab).start()

        @pl.when(c == chunks - 1)
        def _():
            slab = slabs - 1
            for sub in range(q):

                @pl.when(sub != sub_me)
                def _():
                    mirror(0, sub, slab, slabs).start()

                @pl.when(sub == sub_me)
                def _():
                    mirrored[slabs * q + sub] = turned[slab, sub * own : (sub + 1) * own]

    def late_grams(t, part_of):
        if not inside:
            return
        count = blocks // 4

        @pl.when(t < 3)
        def _():
            begin = (2 * (t - 1) + part_of) * count
            lax.fori_loop(begin, begin + count, compute_late, 0)

        @pl.when(t == 3)
        def _():
            begin = blocks // 2 - late_lag // 2 + part_of * (late_lag // 4)
            for w in range(begin, begin + late_lag // 4):
                join(w, 1, 1)

    def late_sends(t):
        if not inside:
            return

        @pl.when((t >= 3) & (t - 3 < per_pass - 1))
        def _():
            send_later(per_pass + t - 2)

    def body():
        out = []

        def add(at, lowest, action):
            out.append((at - int(at), int(at), lowest, action))

        for s in range(2, nbits):
            at = OFFSETS[0] if s == 2 else s - 2 + (OFFSETS[2] if s == nbits - 1 else OFFSETS[1])
            count = 1 << (nbits - 1 - s)
            for i in range(count):
                v = 2 * count - 1 - i
                add(at + SPREAD * i / count, 1 if s == 2 else 0, functools.partial(item, v, s))
        add(nbits + FINISH_AT, 0, finish)
        add(nbits + FINISH_AT + REFLECT_AFTER, 0, reflect)
        for part_of in range(2):
            out.append((GRAMS_AT[part_of], None, 0, functools.partial(lambda which, t: late_grams(t, which), part_of)))
        out.append((GRAMS_AT[2], None, 0, late_sends))
        return sorted(out, key=lambda entry: entry[0])

    turn_body = body()
    last = max(delay for _, delay, _, _ in turn_body if delay is not None)

    def step(t, _):
        for _, delay, lowest, action in turn_body:
            if delay is None:
                action(t)
                continue
            c = t - delay

            @pl.when((c >= lowest) & (c < chunks))
            def _():
                action(c)

        return 0

    lax.fori_loop(1, chunks + last, step, 0)

    sums = 2.0 * tally[...]
    sum_real = jnp.where(paired > 0, sums, 0.0)
    sum_imag = jnp.where(paired > 0, 0.0, sums)
    phase_real = jnp.where(turn == 0, 1.0, jnp.where(turn == 2, -1.0, 0.0))
    phase_imag = jnp.where(turn == 1, 1.0, jnp.where(turn == 3, -1.0, 0.0))
    total = jnp.concatenate(
        [phase_real * sum_real - phase_imag * sum_imag, phase_real * sum_imag + phase_imag * sum_real], 0
    )
    outbox[...] = total
    inbox[me] = total

    def share(d, to):
        return pltpu.make_async_remote_copy(
            src_ref=outbox,
            dst_ref=inbox.at[to],
            send_sem=esend.at[d],
            recv_sem=erecv.at[to],
            device_id=coords((me + d) % n, sizes),
            device_id_type=MESH,
        )

    def share_out(d, _):
        share(d, me).start()
        return 0

    lax.fori_loop(1, n, share_out, 0)

    for k in range(1, slabs + 1):
        for sub in range(q):
            slot = (k - 1) * q + sub
            mirror_from(k, sub, k - 1).wait()
            mirrored[slot] = came[slot]
    for sub in range(q):

        @pl.when(sub != sub_me)
        def _():
            mirror_from(0, sub, slabs).wait()
            mirrored[slabs * q + sub] = came[slabs * q + sub]

    def drain(ident, _):
        pltpu.make_async_remote_copy(
            src_ref=part.at[0],
            dst_ref=land.at[ident],
            send_sem=send_sem.at[ident],
            recv_sem=recv_sem.at[0],
            device_id=coords(partner[0], sizes),
            device_id_type=MESH,
        ).wait_send()
        return 0

    lax.fori_loop(1, n, drain, 0)

    def share_in(d, _):
        share(d, (me + d) % n).wait()
        return 0

    lax.fori_loop(1, n, share_in, 0)

    total = inbox[0]
    for j in range(1, n):
        total = total + inbox[j]
    expect[...] = total


def finish_kernel(sizes, kept, mirrored, expected, real, imag, expect):
    n = sizes[0] * sizes[1] * sizes[2]
    own, order = real.shape
    block = max(own, LANES)
    q = block // own
    blocks = order // block
    slabs = kept.shape[0]
    me = flat_index(sizes)
    mine = me // q
    sub_me = me % q

    def columns(k):
        return pl.ds(pl.multiple_of(((mine + k + blocks) % blocks) * block, block), block)

    def turned(slot, side):
        return jnp.concatenate([mirrored[slot * q + sub][:, side * own : (side + 1) * own] for sub in range(q)], 1)

    for k in range(1, slabs):
        real[:, columns(k)] = kept[k - 1, :, :block]
        imag[:, columns(k)] = kept[k - 1, :, block:]
        real[:, columns(-k)] = turned(k - 1, 0)
        imag[:, columns(-k)] = -turned(k - 1, 1)
    row = sub_me * own + lax.broadcasted_iota(jnp.int32, (own, block), 0)
    lane = lax.broadcasted_iota(jnp.int32, (own, block), 1)
    near, other = kept[slabs - 1, :, :block], turned(slabs, 0)
    real[:, columns(0)] = jnp.where(row <= lane, near, other)
    imag[:, columns(0)] = jnp.where(row > lane, near, jnp.where(row < lane, -other, 0.0))
    far, other = kept[slabs - 1, :, block:], turned(slabs - 1, 1)
    holds = row - lane <= jnp.where(mine < blocks // 2, 0, -1)
    real[:, columns(slabs)] = jnp.where(holds, far, other)
    imag[:, columns(slabs)] = jnp.where(holds, -other, far)
    expect[...] = expected[...]


def on_device(sizes, amplitudes, pauli_x, pauli_z, pauli_phase):
    n = sizes[0] * sizes[1] * sizes[2]
    _, depth, order = amplitudes.shape
    own = order // n
    block = max(own, LANES)
    q = block // own
    blocks = order // block
    slabs = blocks // 2
    group = min(slabs, max(1, LANES // (2 * own)))
    chunks = slabs // group
    width = (slabs + 1) * block
    slots = (slabs + 1) * q
    vmem = pl.BlockSpec(memory_space=pltpu.VMEM)
    terms = pauli_x.shape[0]
    kept, mirrored, expect = pl.pallas_call(
        functools.partial(gram_kernel, sizes, float(depth * n), min(EARLY, chunks // 2)),
        out_shape=(
            jax.ShapeDtypeStruct((slabs, own, 2 * block), jnp.float32),
            jax.ShapeDtypeStruct((slots, own, 2 * own), jnp.float32),
            jax.ShapeDtypeStruct((2, terms), jnp.float32),
        ),
        in_specs=[pl.BlockSpec(memory_space=pl.ANY), vmem, vmem, vmem],
        out_specs=(vmem,) * 3,
        scratch_shapes=[
            pltpu.VMEM((2 * depth, order + width - block), jnp.bfloat16),
            pltpu.VMEM((n, slabs, own, 2 * block), jnp.float32),
            pltpu.VMEM((n, slabs, own, 2 * block), jnp.float32),
            pltpu.VMEM((slabs, block, 2 * own), jnp.float32),
            pltpu.VMEM((slots, own, 2 * own), jnp.float32),
            pltpu.VMEM((6 * own, terms), jnp.bfloat16),
            pltpu.VMEM((1, terms), jnp.float32),
            pltpu.VMEM((2, terms), jnp.float32),
            pltpu.VMEM((n, 2, terms), jnp.float32),
            pltpu.SemaphoreType.DMA((4,)),
            pltpu.SemaphoreType.DMA((n,)),
            pltpu.SemaphoreType.DMA((n * chunks,)),
            pltpu.SemaphoreType.DMA((slots,)),
            pltpu.SemaphoreType.DMA((slots,)),
            pltpu.SemaphoreType.DMA((n,)),
            pltpu.SemaphoreType.DMA((n,)),
        ],
        compiler_params=pltpu.CompilerParams(collective_id=0, has_side_effects=True, vmem_limit_bytes=VMEM_LIMIT),
    )(amplitudes, pauli_x[None], pauli_z[None], pauli_phase[None])
    real, imag, expect = pl.pallas_call(
        functools.partial(finish_kernel, sizes),
        out_shape=(
            jax.ShapeDtypeStruct((own, order), jnp.float32),
            jax.ShapeDtypeStruct((own, order), jnp.float32),
            jax.ShapeDtypeStruct((2, terms), jnp.float32),
        ),
        in_specs=[vmem] * 3,
        out_specs=(vmem,) * 3,
    )(kept, mirrored, expect)
    return real, imag, expect


def solution(mesh):
    sizes = tuple(mesh.shape[axis] for axis in AXES)
    return jax.shard_map(
        functools.partial(on_device, sizes),
        mesh=mesh,
        in_specs=(P(None, AXES, None), P(), P(), P()),
        out_specs=(P(AXES, None), P(AXES, None), P()),
        check_vma=False,
    )
```

```python
import functools

import jax
import jax.numpy as jnp
from jax import lax
from jax.experimental import pallas as pl
from jax.experimental.pallas import tpu as pltpu
from jax.sharding import PartitionSpec as P

AXES = ("gx", "gy", "gz")
LANES = 128
EARLY = 2
OFFSETS = (0.0, 0.246, 0.02)
SPREAD = 0.4
FINISH_AT = 0.124
REFLECT_AFTER = 1.0
GRAMS_AT = (0.28, 0.35, 0.5)
VMEM_LIMIT = 52 << 20
MESH = pl.DeviceIdType.MESH


def log2(value):
    return value.bit_length() - 1


def flat_index(sizes):
    return (lax.axis_index("gx") * sizes[1] + lax.axis_index("gy")) * sizes[2] + lax.axis_index("gz")


def coords(flat, sizes):
    return (flat // (sizes[1] * sizes[2]), (flat // sizes[2]) % sizes[1], flat % sizes[2])


def flip(bit, by):
    return bit + by - 2 * bit * by


def stage_order(sizes):
    zs = log2(sizes[2])
    ys = log2(sizes[1])
    xs = log2(sizes[0])
    rest_x = [zs + ys + t for t in range(xs - 1, 0, -1)]
    rest_y = [zs + t for t in range(ys)]
    rest_z = list(range(zs - 1, -1, -1))
    order = [zs + ys] + rest_x + rest_y[:1] + rest_z + rest_y[1:]
    trade = order.index(rest_z[0]) if rest_x and rest_z else 1
    return order, trade


def parity_sign(masked):
    shift = 16
    while shift >= 1:
        masked = jnp.bitwise_xor(masked, jnp.right_shift(masked, shift))
        shift //= 2
    return (1 - 2 * jnp.bitwise_and(masked, 1)).astype(jnp.float32)


def row_order(sizes, q):
    nbits = log2(sizes[0] * sizes[1] * sizes[2])
    stages, _ = stage_order(sizes)
    lowbits = log2(q)
    return [p for p in stages[2:3] + stages[4:] + stages[1:2] + stages[3:4] if lowbits <= p < nbits]


def early_items(sizes, q, lag, flight):
    nbits = log2(sizes[0] * sizes[1] * sizes[2])
    stages, trade = stage_order(sizes)
    high = row_order(sizes, q)

    def pair_of(v, half):
        by_stage = [(v >> (nbits - 1 - s)) & 1 for s in range(nbits)]
        if half:
            by_stage[1], by_stage[trade] = by_stage[trade], by_stage[1]
        flips = {p: by_stage[s] for s, p in enumerate(stages)}
        w = 0
        for p in high:
            w = 2 * w + 1 - flips[p]
        return w

    out = []
    for v in range((1 << (nbits - 2)) - 1, (1 << (nbits - 3)) - 1, -1):
        waits = []
        for half in range(2):
            waits.append(2 * pair_of(v, half) + 1 + lag)
            waits.append(2 * pair_of(v | (1 << (nbits - 2)), half) + 1 + lag + flight)
        out.append((max(waits), v))
    return sorted(out, key=lambda item: (item[0], -item[1]))


def gram_kernel(
    sizes, total_cols, early, amp, px_in, pz_in, phase_in, kept, mirrored, expect,
    ext, px, pz, phase, part, land, turned, came, spread, tally, outbox, inbox, load_sem, mask_sem, send_sem, recv_sem, msend, mrecv, esend, erecv,
):
    n = sizes[0] * sizes[1] * sizes[2]
    nbits = log2(n)
    depth = amp.shape[1]
    order = amp.shape[2]
    own = order // n
    block = max(own, LANES)
    q = block // own
    blocks = order // block
    width = (blocks // 2 + 1) * block
    slabs = part.shape[1]
    chunks = recv_sem.shape[0] // n
    group = slabs // chunks
    passes = 2
    per_pass = chunks // passes
    part_slabs = slabs // passes
    me = flat_index(sizes)
    bits = [(me // (1 << p)) % 2 for p in range(nbits)]
    stages, trade = stage_order(sizes)
    half = bits[stages[0]]
    lag, late_lag, flight = 4, blocks // 2, 6

    def loads():
        out = []
        for part_index in range(2):
            rows = pl.ds(part_index * depth, depth)
            out.append(pltpu.make_async_copy(amp.at[part_index], ext.at[rows, pl.ds(0, order)], load_sem.at[2 * part_index]))
            out.append(
                pltpu.make_async_copy(
                    amp.at[part_index, :, pl.ds(0, width - block)],
                    ext.at[rows, pl.ds(order, width - block)],
                    load_sem.at[2 * part_index + 1],
                )
            )
        return out


    def flips_of(v):
        by_stage = [(v >> (nbits - 1 - s)) & 1 for s in range(nbits)]
        flips = [0] * nbits
        for s, p in enumerate(stages):
            flips[p] = by_stage[s]
        flips[stages[1]] = by_stage[1] * (1 - half) + by_stage[trade] * half
        flips[stages[trade]] = by_stage[trade] * (1 - half) + by_stage[1] * half
        return flips

    def place(flips):
        return sum((1 << p) * flip(bits[p], flips[p]) for p in range(nbits))

    def name(flips):
        return sum((1 << p) * flips[p] for p in range(nbits))

    partner = [place(flips_of(1 << (nbits - 1 - s))) for s in range(nbits)]
    barrier = pltpu.get_barrier_semaphore()
    for other in partner:
        pl.semaphore_signal(barrier, inc=1, device_id=coords(other, sizes), device_id_type=MESH)
    for copy in loads():
        copy.start()
    masks = [
        pltpu.make_async_copy(source, target, mask_sem.at[i])
        for i, (source, target) in enumerate(((px_in, px), (pz_in, pz), (phase_in, phase)))
    ]
    for copy in masks:
        copy.start()
    lowbits = log2(q)
    high = row_order(sizes, q)

    def message(where, ident, target, c):
        piece = pl.ds(c * group, group)
        return pltpu.make_async_remote_copy(
            src_ref=part.at[where, piece],
            dst_ref=land.at[ident, piece],
            send_sem=send_sem.at[ident],
            recv_sem=recv_sem.at[ident * chunks + c],
            device_id=coords(target, sizes),
            device_id_type=MESH,
        )

    def across(where, ident, which):
        piece = pl.ds(which * part_slabs, part_slabs)
        return pltpu.make_async_remote_copy(
            src_ref=part.at[where, piece],
            dst_ref=land.at[ident, piece],
            send_sem=send_sem.at[ident],
            recv_sem=recv_sem.at[ident * chunks + which],
            device_id=coords(partner[0], sizes),
            device_id_type=MESH,
        )

    def row_block(u):
        flips = [0] * nbits
        flips[stages[0]] = 1 - u % 2
        for j, p in enumerate(high):
            flips[p] = 1 - (u // (1 << (len(high) - j))) % 2
        return flips

    def with_low(flips, g):
        return [(g >> p) & 1 if p < lowbits else flips[p] for p in range(nbits)]

    def summed(where, names, slab, rows):
        total = part[where, slab, rows, :]
        for ident in names:
            total = total + land[ident, slab, rows, :]
        return total

    def join(w, which, upto):
        for g in range(q):
            flips = with_low(row_block(2 * w + 1), g)
            where, ident = place(flips), name(flips)
            across(where, ident + (1 << stages[0]), which).wait_recv()
            for slab in range(which * part_slabs, (which + 1) * part_slabs):
                for r in range(0, own, 8):
                    rows = pl.ds(r, 8)
                    part[where, slab, rows, :] = summed(where, [ident + (1 << stages[0])], slab, rows)
        for c in range(which * per_pass, which * per_pass + upto):
            send_first(w, c)

    def send_first(w, c):
        for g in range(q):
            flips = with_low(row_block(2 * w + 1), g)
            goes = flips[stages[1]] * (1 - half) + flips[stages[trade]] * half

            @pl.when(goes == 1)
            def _():
                message(place(flips), name(flips), partner[1], c).start()

    def arrive(v, upto, c):
        names = [name(flips_of(v | (1 << (nbits - 1 - t)))) for t in range(1, upto)]
        for ident in names:
            message(0, ident, partner[0], c).wait_recv()
        return names

    def item(v, s, c):
        names = arrive(v, s, c)
        flips = flips_of(v)
        where = place(flips)
        for g in range(group):
            slab = c * group + g
            for r in range(0, own, 8):
                rows = pl.ds(r, 8)
                part[where, slab, rows, :] = summed(where, names, slab, rows)
        message(where, name(flips), partner[s], c).start()

    terms = px.shape[1]
    mine = me // q
    sub_me = me % q
    base = me * own

    for copy in loads():
        copy.wait()

    row_in = lax.broadcasted_iota(jnp.int32, (block, block), 0)
    lane_in = lax.broadcasted_iota(jnp.int32, (block, block), 1)
    seconds = early_items(sizes, q, lag, flight)

    def gram(u, which):
        flips = row_block(u)
        first = sum((1 << p) * flip(bits[p], flips[p]) for p in range(lowbits, nbits))
        start = pl.multiple_of(first * own, block)
        lhs = ext[:, pl.ds(start, block)]
        crossed = jnp.concatenate([lhs[depth:], -lhs[:depth]], 0)
        both = jnp.concatenate([lhs, crossed], 1)

        def product(k, count):
            rhs = ext[:, pl.ds(pl.multiple_of(start + k * block, block), count * block)]
            return lax.dot_general(both, rhs, (((0,), (0,)), ((), ())), preferred_element_type=jnp.float32)

        low = which * part_slabs
        rows = product(low + 1, part_slabs)
        closing = which == passes - 1
        plain = part_slabs - 1 if closing else part_slabs
        if closing:
            here = product(0, 1)
            far_cols = slice(plain * block, (plain + 1) * block)
            bound = jnp.where(first // q < blocks // 2, 0, -1)
            near = jnp.where(row_in - lane_in <= 0, here[:block], here[block:])
            far = jnp.where(row_in - lane_in <= bound, rows[:block, far_cols], rows[block:, far_cols])
        for sub in range(q):
            at = slice(sub * own, (sub + 1) * own)
            more = slice(block + sub * own, block + (sub + 1) * own)
            for k in range(plain):
                cols = slice(k * block, (k + 1) * block)
                part[first + sub, low + k, :, 0:block] = rows[at, cols]
                part[first + sub, low + k, :, block : 2 * block] = rows[more, cols]
            if closing:
                part[first + sub, slabs - 1, :, 0:block] = near[at]
                part[first + sub, slabs - 1, :, block : 2 * block] = far[at]

    def hand_over(u, which):
        for g in range(q):
            flips = with_low(row_block(u), g)
            across(place(flips), name(flips), which).start()

    def compute(u, _):
        @pl.when(u == 1)
        def _():
            pl.semaphore_wait(barrier, nbits)

        @pl.when(u % 2 == 1)
        def _():
            hand_over(u - 1, 0)

        @pl.when((u % 2 == 1) & (u >= 1 + lag))
        def _():
            join((u - lag) // 2, 0, early)

        for at in sorted({at for at, _ in seconds if at < blocks}):

            @pl.when(u == at)
            def _():
                for when, v in seconds:
                    if when == at:
                        item(v, 2, 0)

        gram(u, 0)
        return 0

    def compute_late(u, _):
        @pl.when(u % 2 == 1)
        def _():
            hand_over(u - 1, 1)

        @pl.when((u % 2 == 1) & (u >= 1 + late_lag))
        def _():
            join((u - late_lag) // 2, 1, 1)

        gram(u, 1)
        return 0

    def send_later(c):
        for w in range(blocks // 2):
            send_first(w, c)

    lax.fori_loop(0, blocks, compute, 0)

    for w in range(max(blocks // 2 - lag // 2, 0), blocks // 2):
        join(w, 0, early)
    for at, v in seconds:
        if at >= blocks:
            item(v, 2, 0)
    for c in range(early, per_pass):
        send_later(c)

    inside = per_pass >= 4
    if not inside:
        lax.fori_loop(0, blocks, compute_late, 0)
        for w in range(max(blocks // 2 - late_lag // 2, 0), blocks // 2):
            join(w, 1, per_pass)

    for copy in masks:
        copy.wait()
    turn = phase[...]
    paired = parity_sign(jnp.bitwise_and(px[...], pz[...]))
    wanted = jnp.bitwise_xor(px[...], base)
    lane_terms = lax.broadcasted_iota(jnp.int32, (block, terms), 0)
    row = lax.broadcasted_iota(jnp.int32, (own, block), 0)
    lane = lax.broadcasted_iota(jnp.int32, (own, block), 1)
    ids = base + lax.broadcasted_iota(jnp.int32, (own, terms), 0)
    signs = parity_sign(jnp.bitwise_and(ids, pz[...]))
    signs_real = jnp.where(paired > 0, signs, 0.0)
    signs_imag = jnp.where(paired > 0, 0.0, signs)
    spread[...] = jnp.concatenate([signs_real] * 3 + [signs_imag] * 3, 0).astype(jnp.bfloat16)
    tally[...] = jnp.zeros_like(tally)

    def swapped_rows(values):
        for p in range(log2(own)):
            step = 1 << p
            swapped = jnp.where(
                jnp.bitwise_and(lane, step) != 0,
                pltpu.roll(values, step, 1),
                pltpu.roll(values, block - step, 1),
            )
            values = jnp.where(jnp.bitwise_and(row, step) != 0, swapped, values)
        return values

    def in_three(values):
        high_part = values.astype(jnp.bfloat16)
        rest = values - high_part.astype(jnp.float32)
        middle = rest.astype(jnp.bfloat16)
        low = (rest - middle.astype(jnp.float32)).astype(jnp.bfloat16)
        return [high_part, middle, low]

    def pick(real_values, imag_values, k):
        stacked = jnp.concatenate(in_three(swapped_rows(real_values)) + in_three(swapped_rows(imag_values)), 0)
        sums = lax.dot_general(stacked, spread[...], (((0,), (0,)), ((), ())), preferred_element_type=jnp.float32)
        chosen = jnp.where(lane_terms + ((mine + k) % blocks) * block == wanted, sums, 0.0)
        tally[...] = tally[...] + jnp.sum(chosen, axis=0, keepdims=True)

    def mirror(k, sub, source, slot):
        return pltpu.make_async_remote_copy(
            src_ref=turned.at[source, pl.ds(sub * own, own)],
            dst_ref=came.at[slot * q + sub_me],
            send_sem=msend.at[slot * q + sub],
            recv_sem=mrecv.at[slot * q + sub_me],
            device_id=coords(((mine + k) % blocks) * q + sub, sizes),
            device_id_type=MESH,
        )

    def mirror_from(k, sub, slot):
        return pltpu.make_async_remote_copy(
            src_ref=turned.at[0, pl.ds(sub * own, own)],
            dst_ref=came.at[slot * q + sub],
            send_sem=msend.at[slot * q + sub],
            recv_sem=mrecv.at[slot * q + sub],
            device_id=coords(((mine + k) % blocks) * q + sub, sizes),
            device_id_type=MESH,
        )

    local_row = sub_me * own + row
    bound_me = jnp.where(mine < blocks // 2, 0, -1)

    def finish(c):
        names = arrive(0, nbits, c)
        for g in range(group):
            slab = c * group + g
            for r in range(0, own, 8):
                rows = pl.ds(r, 8)
                kept[slab, rows, :] = summed(me, names, slab, rows) / total_cols
            turned[slab] = jnp.concatenate([kept[slab, :, :block], kept[slab, :, block:]], 0).T

            @pl.when(slab < slabs - 1)
            def _():
                pick(kept[slab, :, :block], kept[slab, :, block:], slab + 1)

        @pl.when(c == chunks - 1)
        def _():
            slab = slabs - 1
            near = kept[slab, :, :block]
            upper = jnp.where(local_row < lane, near, jnp.where(local_row == lane, 0.5 * near, 0.0))
            pick(upper, jnp.where(local_row > lane, near, 0.0), 0)
            far = kept[slab, :, block:]
            holds = local_row - lane <= bound_me
            pick(jnp.where(holds, far, 0.0), jnp.where(holds, 0.0, far), slabs)

    def reflect(c):
        for g in range(group):
            slab = c * group + g
            for sub in range(q):
                mirror(slab + 1, sub, slab, slab).start()

        @pl.when(c == chunks - 1)
        def _():
            slab = slabs - 1
            for sub in range(q):

                @pl.when(sub != sub_me)
                def _():
                    mirror(0, sub, slab, slabs).start()

                @pl.when(sub == sub_me)
                def _():
                    mirrored[slabs * q + sub] = turned[slab, sub * own : (sub + 1) * own]

    def late_grams(t, part_of):
        if not inside:
            return
        count = blocks // 4

        @pl.when(t < 3)
        def _():
            begin = (2 * (t - 1) + part_of) * count
            lax.fori_loop(begin, begin + count, compute_late, 0)

        @pl.when(t == 3)
        def _():
            begin = blocks // 2 - late_lag // 2 + part_of * (late_lag // 4)
            for w in range(begin, begin + late_lag // 4):
                join(w, 1, 1)

    def late_sends(t):
        if not inside:
            return

        @pl.when((t >= 3) & (t - 3 < per_pass - 1))
        def _():
            send_later(per_pass + t - 2)

    def body():
        out = []

        def add(at, lowest, action):
            out.append((at - int(at), int(at), lowest, action))

        for s in range(2, nbits):
            at = OFFSETS[0] if s == 2 else s - 2 + (OFFSETS[2] if s == nbits - 1 else OFFSETS[1])
            count = 1 << (nbits - 1 - s)
            for i in range(count):
                v = 2 * count - 1 - i
                add(at + SPREAD * i / count, 1 if s == 2 else 0, functools.partial(item, v, s))
        add(nbits + FINISH_AT, 0, finish)
        add(nbits + FINISH_AT + REFLECT_AFTER, 0, reflect)
        for part_of in range(2):
            out.append((GRAMS_AT[part_of], None, 0, functools.partial(lambda which, t: late_grams(t, which), part_of)))
        out.append((GRAMS_AT[2], None, 0, late_sends))
        return sorted(out, key=lambda entry: entry[0])

    turn_body = body()
    last = max(delay for _, delay, _, _ in turn_body if delay is not None)

    def step(t, _):
        for _, delay, lowest, action in turn_body:
            if delay is None:
                action(t)
                continue
            c = t - delay

            @pl.when((c >= lowest) & (c < chunks))
            def _():
                action(c)

        return 0

    lax.fori_loop(1, chunks + last, step, 0)

    sums = 2.0 * tally[...]
    sum_real = jnp.where(paired > 0, sums, 0.0)
    sum_imag = jnp.where(paired > 0, 0.0, sums)
    phase_real = jnp.where(turn == 0, 1.0, jnp.where(turn == 2, -1.0, 0.0))
    phase_imag = jnp.where(turn == 1, 1.0, jnp.where(turn == 3, -1.0, 0.0))
    total = jnp.concatenate(
        [phase_real * sum_real - phase_imag * sum_imag, phase_real * sum_imag + phase_imag * sum_real], 0
    )
    outbox[...] = total
    inbox[me] = total

    def share(d, to):
        return pltpu.make_async_remote_copy(
            src_ref=outbox,
            dst_ref=inbox.at[to],
            send_sem=esend.at[d],
            recv_sem=erecv.at[to],
            device_id=coords((me + d) % n, sizes),
            device_id_type=MESH,
        )

    def share_out(d, _):
        share(d, me).start()
        return 0

    lax.fori_loop(1, n, share_out, 0)

    for k in range(1, slabs + 1):
        for sub in range(q):
            slot = (k - 1) * q + sub
            mirror_from(k, sub, k - 1).wait()
            mirrored[slot] = came[slot]
    for sub in range(q):

        @pl.when(sub != sub_me)
        def _():
            mirror_from(0, sub, slabs).wait()
            mirrored[slabs * q + sub] = came[slabs * q + sub]

    def drain(ident, _):
        pltpu.make_async_remote_copy(
            src_ref=part.at[0],
            dst_ref=land.at[ident],
            send_sem=send_sem.at[ident],
            recv_sem=recv_sem.at[0],
            device_id=coords(partner[0], sizes),
            device_id_type=MESH,
        ).wait_send()
        return 0

    lax.fori_loop(1, n, drain, 0)

    def share_in(d, _):
        share(d, (me + d) % n).wait()
        return 0

    lax.fori_loop(1, n, share_in, 0)

    total = inbox[0]
    for j in range(1, n):
        total = total + inbox[j]
    expect[...] = total


def finish_kernel(sizes, kept, mirrored, expected, real, imag, expect):
    n = sizes[0] * sizes[1] * sizes[2]
    own, order = real.shape
    block = max(own, LANES)
    q = block // own
    blocks = order // block
    slabs = kept.shape[0]
    me = flat_index(sizes)
    mine = me // q
    sub_me = me % q

    def columns(k):
        return pl.ds(pl.multiple_of(((mine + k + blocks) % blocks) * block, block), block)

    def turned(slot, side):
        return jnp.concatenate([mirrored[slot * q + sub][:, side * own : (side + 1) * own] for sub in range(q)], 1)

    for k in range(1, slabs):
        real[:, columns(k)] = kept[k - 1, :, :block]
        imag[:, columns(k)] = kept[k - 1, :, block:]
        real[:, columns(-k)] = turned(k - 1, 0)
        imag[:, columns(-k)] = -turned(k - 1, 1)
    row = sub_me * own + lax.broadcasted_iota(jnp.int32, (own, block), 0)
    lane = lax.broadcasted_iota(jnp.int32, (own, block), 1)
    near, other = kept[slabs - 1, :, :block], turned(slabs, 0)
    real[:, columns(0)] = jnp.where(row <= lane, near, other)
    imag[:, columns(0)] = jnp.where(row > lane, near, jnp.where(row < lane, -other, 0.0))
    far, other = kept[slabs - 1, :, block:], turned(slabs - 1, 1)
    holds = row - lane <= jnp.where(mine < blocks // 2, 0, -1)
    real[:, columns(slabs)] = jnp.where(holds, far, other)
    imag[:, columns(slabs)] = jnp.where(holds, -other, far)
    expect[...] = expected[...]


def on_device(sizes, amplitudes, pauli_x, pauli_z, pauli_phase):
    n = sizes[0] * sizes[1] * sizes[2]
    _, depth, order = amplitudes.shape
    own = order // n
    block = max(own, LANES)
    q = block // own
    blocks = order // block
    slabs = blocks // 2
    group = min(slabs, max(1, LANES // (2 * own)))
    chunks = slabs // group
    width = (slabs + 1) * block
    slots = (slabs + 1) * q
    vmem = pl.BlockSpec(memory_space=pltpu.VMEM)
    terms = pauli_x.shape[0]
    kept, mirrored, expect = pl.pallas_call(
        functools.partial(gram_kernel, sizes, float(depth * n), min(EARLY, chunks // 2)),
        out_shape=(
            jax.ShapeDtypeStruct((slabs, own, 2 * block), jnp.float32),
            jax.ShapeDtypeStruct((slots, own, 2 * own), jnp.float32),
            jax.ShapeDtypeStruct((2, terms), jnp.float32),
        ),
        in_specs=[pl.BlockSpec(memory_space=pltpu.HBM)] * 4,
        out_specs=(vmem,) * 3,
        scratch_shapes=[
            pltpu.VMEM((2 * depth, order + width - block), jnp.bfloat16),
            *[pltpu.VMEM((1, terms), jnp.int32)] * 3,
            pltpu.VMEM((n, slabs, own, 2 * block), jnp.float32),
            pltpu.VMEM((n, slabs, own, 2 * block), jnp.float32),
            pltpu.VMEM((slabs, block, 2 * own), jnp.float32),
            pltpu.VMEM((slots, own, 2 * own), jnp.float32),
            pltpu.VMEM((6 * own, terms), jnp.bfloat16),
            pltpu.VMEM((1, terms), jnp.float32),
            pltpu.VMEM((2, terms), jnp.float32),
            pltpu.VMEM((n, 2, terms), jnp.float32),
            pltpu.SemaphoreType.DMA((4,)),
            pltpu.SemaphoreType.DMA((3,)),
            pltpu.SemaphoreType.DMA((n,)),
            pltpu.SemaphoreType.DMA((n * chunks,)),
            pltpu.SemaphoreType.DMA((slots,)),
            pltpu.SemaphoreType.DMA((slots,)),
            pltpu.SemaphoreType.DMA((n,)),
            pltpu.SemaphoreType.DMA((n,)),
        ],
        compiler_params=pltpu.CompilerParams(collective_id=0, has_side_effects=True, vmem_limit_bytes=VMEM_LIMIT),
    )(amplitudes, *[pltpu.with_memory_space_constraint(m[None], pltpu.HBM) for m in (pauli_x, pauli_z, pauli_phase)])
    real, imag, expect = pl.pallas_call(
        functools.partial(finish_kernel, sizes),
        out_shape=(
            jax.ShapeDtypeStruct((own, order), jnp.float32),
            jax.ShapeDtypeStruct((own, order), jnp.float32),
            jax.ShapeDtypeStruct((2, terms), jnp.float32),
        ),
        in_specs=[vmem] * 3,
        out_specs=(vmem,) * 3,
        compiler_params=pltpu.CompilerParams(vmem_limit_bytes=8 << 20),
    )(kept, mirrored, expect)
    return real, imag, expect


def solution(mesh):
    sizes = tuple(mesh.shape[axis] for axis in AXES)
    return jax.shard_map(
        functools.partial(on_device, sizes),
        mesh=mesh,
        in_specs=(P(None, AXES, None), P(), P(), P()),
        out_specs=(P(AXES, None), P(AXES, None), P()),
        check_vma=False,
    )
```

```python
import functools

import jax
import jax.numpy as jnp
from jax import lax
from jax.experimental import pallas as pl
from jax.experimental.pallas import tpu as pltpu
from jax.sharding import PartitionSpec as P

AXES = ("gx", "gy", "gz")
LANES = 128
EARLY = 2
OFFSETS = (0.0, 0.246, 0.02)
SPREAD = 0.4
FINISH_AT = 0.124
REFLECT_AFTER = 1.0
GRAMS_AT = (0.28, 0.35, 0.5)
VMEM_LIMIT = 52 << 20
MESH = pl.DeviceIdType.MESH


def log2(value):
    return value.bit_length() - 1


def flat_index(sizes):
    return (lax.axis_index("gx") * sizes[1] + lax.axis_index("gy")) * sizes[2] + lax.axis_index("gz")


def coords(flat, sizes):
    return (flat // (sizes[1] * sizes[2]), (flat // sizes[2]) % sizes[1], flat % sizes[2])


def flip(bit, by):
    return bit + by - 2 * bit * by


def stage_order(sizes):
    zs = log2(sizes[2])
    ys = log2(sizes[1])
    xs = log2(sizes[0])
    rest_x = [zs + ys + t for t in range(xs - 1, 0, -1)]
    rest_y = [zs + t for t in range(ys)]
    rest_z = list(range(zs - 1, -1, -1))
    order = [zs + ys] + rest_x + rest_y[:1] + rest_z + rest_y[1:]
    trade = order.index(rest_z[0]) if rest_x and rest_z else 1
    return order, trade


def parity_sign(masked):
    shift = 16
    while shift >= 1:
        masked = jnp.bitwise_xor(masked, jnp.right_shift(masked, shift))
        shift //= 2
    return (1 - 2 * jnp.bitwise_and(masked, 1)).astype(jnp.float32)


def row_order(sizes, q):
    nbits = log2(sizes[0] * sizes[1] * sizes[2])
    stages, _ = stage_order(sizes)
    lowbits = log2(q)
    return [p for p in stages[2:3] + stages[4:] + stages[1:2] + stages[3:4] if lowbits <= p < nbits]


def early_items(sizes, q, lag, flight):
    nbits = log2(sizes[0] * sizes[1] * sizes[2])
    stages, trade = stage_order(sizes)
    high = row_order(sizes, q)

    def pair_of(v, half):
        by_stage = [(v >> (nbits - 1 - s)) & 1 for s in range(nbits)]
        if half:
            by_stage[1], by_stage[trade] = by_stage[trade], by_stage[1]
        flips = {p: by_stage[s] for s, p in enumerate(stages)}
        w = 0
        for p in high:
            w = 2 * w + 1 - flips[p]
        return w

    out = []
    for v in range((1 << (nbits - 2)) - 1, (1 << (nbits - 3)) - 1, -1):
        waits = []
        for half in range(2):
            waits.append(2 * pair_of(v, half) + 1 + lag)
            waits.append(2 * pair_of(v | (1 << (nbits - 2)), half) + 1 + lag + flight)
        out.append((max(waits), v))
    return sorted(out, key=lambda item: (item[0], -item[1]))


def gram_kernel(
    sizes, total_cols, early, amp, px_in, pz_in, phase_in, kept, mirrored, expect,
    ext, px, pz, phase, part, land, turned, came, spread, tally, outbox, inbox, load_sem, mask_sem, send_sem, recv_sem, msend, mrecv, esend, erecv,
):
    n = sizes[0] * sizes[1] * sizes[2]
    nbits = log2(n)
    depth = amp.shape[1]
    order = amp.shape[2]
    own = order // n
    block = max(own, LANES)
    q = block // own
    blocks = order // block
    width = (blocks // 2 + 1) * block
    slabs = part.shape[1]
    chunks = recv_sem.shape[0] // n
    group = slabs // chunks
    passes = 2
    per_pass = chunks // passes
    part_slabs = slabs // passes
    me = flat_index(sizes)
    bits = [(me // (1 << p)) % 2 for p in range(nbits)]
    stages, trade = stage_order(sizes)
    half = bits[stages[0]]
    lag, late_lag, flight = 4, blocks // 2, 6

    wrap = part_slabs * block

    def loads():
        out = []
        for part_index in range(2):
            rows = pl.ds(part_index * depth, depth)
            out.append(pltpu.make_async_copy(amp.at[part_index], ext.at[rows, pl.ds(0, order)], load_sem.at[2 * part_index]))
            out.append(
                pltpu.make_async_copy(
                    amp.at[part_index, :, pl.ds(0, wrap)],
                    ext.at[rows, pl.ds(order, wrap)],
                    load_sem.at[2 * part_index + 1],
                )
            )
        for part_index in range(2):
            out.append(
                pltpu.make_async_copy(
                    amp.at[part_index, :, pl.ds(wrap, width - block - wrap)],
                    ext.at[pl.ds(part_index * depth, depth), pl.ds(order + wrap, width - block - wrap)],
                    load_sem.at[4 + part_index],
                )
            )
        return out

    def flips_of(v):
        by_stage = [(v >> (nbits - 1 - s)) & 1 for s in range(nbits)]
        flips = [0] * nbits
        for s, p in enumerate(stages):
            flips[p] = by_stage[s]
        flips[stages[1]] = by_stage[1] * (1 - half) + by_stage[trade] * half
        flips[stages[trade]] = by_stage[trade] * (1 - half) + by_stage[1] * half
        return flips

    def place(flips):
        return sum((1 << p) * flip(bits[p], flips[p]) for p in range(nbits))

    def name(flips):
        return sum((1 << p) * flips[p] for p in range(nbits))

    partner = [place(flips_of(1 << (nbits - 1 - s))) for s in range(nbits)]
    barrier = pltpu.get_barrier_semaphore()
    for other in partner:
        pl.semaphore_signal(barrier, inc=1, device_id=coords(other, sizes), device_id_type=MESH)
    for copy in loads():
        copy.start()
    masks = [
        pltpu.make_async_copy(source, target, mask_sem.at[i])
        for i, (source, target) in enumerate(((px_in, px), (pz_in, pz), (phase_in, phase)))
    ]
    for copy in masks:
        copy.start()
    lowbits = log2(q)
    high = row_order(sizes, q)

    def message(where, ident, target, c):
        piece = pl.ds(c * group, group)
        return pltpu.make_async_remote_copy(
            src_ref=part.at[where, piece],
            dst_ref=land.at[ident, piece],
            send_sem=send_sem.at[ident],
            recv_sem=recv_sem.at[ident * chunks + c],
            device_id=coords(target, sizes),
            device_id_type=MESH,
        )

    def across(where, ident, which):
        piece = pl.ds(which * part_slabs, part_slabs)
        return pltpu.make_async_remote_copy(
            src_ref=part.at[where, piece],
            dst_ref=land.at[ident, piece],
            send_sem=send_sem.at[ident],
            recv_sem=recv_sem.at[ident * chunks + which],
            device_id=coords(partner[0], sizes),
            device_id_type=MESH,
        )

    def row_block(u):
        flips = [0] * nbits
        flips[stages[0]] = 1 - u % 2
        for j, p in enumerate(high):
            flips[p] = 1 - (u // (1 << (len(high) - j))) % 2
        return flips

    def with_low(flips, g):
        return [(g >> p) & 1 if p < lowbits else flips[p] for p in range(nbits)]

    def summed(where, names, slab, rows):
        total = part[where, slab, rows, :]
        for ident in names:
            total = total + land[ident, slab, rows, :]
        return total

    def join(w, which, upto):
        for g in range(q):
            flips = with_low(row_block(2 * w + 1), g)
            where, ident = place(flips), name(flips)
            across(where, ident + (1 << stages[0]), which).wait_recv()
            for slab in range(which * part_slabs, (which + 1) * part_slabs):
                for r in range(0, own, 8):
                    rows = pl.ds(r, 8)
                    part[where, slab, rows, :] = summed(where, [ident + (1 << stages[0])], slab, rows)
        for c in range(which * per_pass, which * per_pass + upto):
            send_first(w, c)

    def send_first(w, c):
        for g in range(q):
            flips = with_low(row_block(2 * w + 1), g)
            goes = flips[stages[1]] * (1 - half) + flips[stages[trade]] * half

            @pl.when(goes == 1)
            def _():
                message(place(flips), name(flips), partner[1], c).start()

    def arrive(v, upto, c):
        names = [name(flips_of(v | (1 << (nbits - 1 - t)))) for t in range(1, upto)]
        for ident in names:
            message(0, ident, partner[0], c).wait_recv()
        return names

    def item(v, s, c):
        names = arrive(v, s, c)
        flips = flips_of(v)
        where = place(flips)
        for g in range(group):
            slab = c * group + g
            for r in range(0, own, 8):
                rows = pl.ds(r, 8)
                part[where, slab, rows, :] = summed(where, names, slab, rows)
        message(where, name(flips), partner[s], c).start()

    terms = px.shape[1]
    mine = me // q
    sub_me = me % q
    base = me * own

    for copy in loads()[:4]:
        copy.wait()

    row_in = lax.broadcasted_iota(jnp.int32, (block, block), 0)
    lane_in = lax.broadcasted_iota(jnp.int32, (block, block), 1)
    seconds = early_items(sizes, q, lag, flight)

    def gram(u, which):
        flips = row_block(u)
        first = sum((1 << p) * flip(bits[p], flips[p]) for p in range(lowbits, nbits))
        start = pl.multiple_of(first * own, block)
        lhs = ext[:, pl.ds(start, block)]
        crossed = jnp.concatenate([lhs[depth:], -lhs[:depth]], 0)
        both = jnp.concatenate([lhs, crossed], 1)

        def product(k, count):
            rhs = ext[:, pl.ds(pl.multiple_of(start + k * block, block), count * block)]
            return lax.dot_general(both, rhs, (((0,), (0,)), ((), ())), preferred_element_type=jnp.float32)

        low = which * part_slabs
        rows = product(low + 1, part_slabs)
        closing = which == passes - 1
        plain = part_slabs - 1 if closing else part_slabs
        if closing:
            here = product(0, 1)
            far_cols = slice(plain * block, (plain + 1) * block)
            bound = jnp.where(first // q < blocks // 2, 0, -1)
            near = jnp.where(row_in - lane_in <= 0, here[:block], here[block:])
            far = jnp.where(row_in - lane_in <= bound, rows[:block, far_cols], rows[block:, far_cols])
        for sub in range(q):
            at = slice(sub * own, (sub + 1) * own)
            more = slice(block + sub * own, block + (sub + 1) * own)
            for k in range(plain):
                cols = slice(k * block, (k + 1) * block)
                part[first + sub, low + k, :, 0:block] = rows[at, cols]
                part[first + sub, low + k, :, block : 2 * block] = rows[more, cols]
            if closing:
                part[first + sub, slabs - 1, :, 0:block] = near[at]
                part[first + sub, slabs - 1, :, block : 2 * block] = far[at]

    def hand_over(u, which):
        for g in range(q):
            flips = with_low(row_block(u), g)
            across(place(flips), name(flips), which).start()

    def compute(u, _):
        @pl.when(u == 1)
        def _():
            pl.semaphore_wait(barrier, nbits)

        @pl.when(u % 2 == 1)
        def _():
            hand_over(u - 1, 0)

        @pl.when((u % 2 == 1) & (u >= 1 + lag))
        def _():
            join((u - lag) // 2, 0, early)

        for at in sorted({at for at, _ in seconds if at < blocks}):

            @pl.when(u == at)
            def _():
                for when, v in seconds:
                    if when == at:
                        item(v, 2, 0)

        gram(u, 0)
        return 0

    def compute_late(u, _):
        @pl.when(u % 2 == 1)
        def _():
            hand_over(u - 1, 1)

        @pl.when((u % 2 == 1) & (u >= 1 + late_lag))
        def _():
            join((u - late_lag) // 2, 1, 1)

        gram(u, 1)
        return 0

    def send_later(c):
        for w in range(blocks // 2):
            send_first(w, c)

    lax.fori_loop(0, blocks, compute, 0)
    for copy in loads()[4:]:
        copy.wait()

    for w in range(max(blocks // 2 - lag // 2, 0), blocks // 2):
        join(w, 0, early)
    for at, v in seconds:
        if at >= blocks:
            item(v, 2, 0)
    for c in range(early, per_pass):
        send_later(c)

    inside = per_pass >= 4
    if not inside:
        lax.fori_loop(0, blocks, compute_late, 0)
        for w in range(max(blocks // 2 - late_lag // 2, 0), blocks // 2):
            join(w, 1, per_pass)

    for copy in masks:
        copy.wait()
    turn = phase[...]
    paired = parity_sign(jnp.bitwise_and(px[...], pz[...]))
    wanted = jnp.bitwise_xor(px[...], base)
    lane_terms = lax.broadcasted_iota(jnp.int32, (block, terms), 0)
    row = lax.broadcasted_iota(jnp.int32, (own, block), 0)
    lane = lax.broadcasted_iota(jnp.int32, (own, block), 1)
    ids = base + lax.broadcasted_iota(jnp.int32, (own, terms), 0)
    signs = parity_sign(jnp.bitwise_and(ids, pz[...]))
    signs_real = jnp.where(paired > 0, signs, 0.0)
    signs_imag = jnp.where(paired > 0, 0.0, signs)
    spread[...] = jnp.concatenate([signs_real] * 3 + [signs_imag] * 3, 0).astype(jnp.bfloat16)
    tally[...] = jnp.zeros_like(tally)

    def swapped_rows(values):
        for p in range(log2(own)):
            step = 1 << p
            swapped = jnp.where(
                jnp.bitwise_and(lane, step) != 0,
                pltpu.roll(values, step, 1),
                pltpu.roll(values, block - step, 1),
            )
            values = jnp.where(jnp.bitwise_and(row, step) != 0, swapped, values)
        return values

    def in_three(values):
        high_part = values.astype(jnp.bfloat16)
        rest = values - high_part.astype(jnp.float32)
        middle = rest.astype(jnp.bfloat16)
        low = (rest - middle.astype(jnp.float32)).astype(jnp.bfloat16)
        return [high_part, middle, low]

    def pick(real_values, imag_values, k):
        stacked = jnp.concatenate(in_three(swapped_rows(real_values)) + in_three(swapped_rows(imag_values)), 0)
        sums = lax.dot_general(stacked, spread[...], (((0,), (0,)), ((), ())), preferred_element_type=jnp.float32)
        chosen = jnp.where(lane_terms + ((mine + k) % blocks) * block == wanted, sums, 0.0)
        tally[...] = tally[...] + jnp.sum(chosen, axis=0, keepdims=True)

    def mirror(k, sub, source, slot):
        return pltpu.make_async_remote_copy(
            src_ref=turned.at[source, pl.ds(sub * own, own)],
            dst_ref=came.at[slot * q + sub_me],
            send_sem=msend.at[slot * q + sub],
            recv_sem=mrecv.at[slot * q + sub_me],
            device_id=coords(((mine + k) % blocks) * q + sub, sizes),
            device_id_type=MESH,
        )

    def mirror_from(k, sub, slot):
        return pltpu.make_async_remote_copy(
            src_ref=turned.at[0, pl.ds(sub * own, own)],
            dst_ref=came.at[slot * q + sub],
            send_sem=msend.at[slot * q + sub],
            recv_sem=mrecv.at[slot * q + sub],
            device_id=coords(((mine + k) % blocks) * q + sub, sizes),
            device_id_type=MESH,
        )

    local_row = sub_me * own + row
    bound_me = jnp.where(mine < blocks // 2, 0, -1)

    def finish(c):
        names = arrive(0, nbits, c)
        for g in range(group):
            slab = c * group + g
            for r in range(0, own, 8):
                rows = pl.ds(r, 8)
                kept[slab, rows, :] = summed(me, names, slab, rows) / total_cols
            turned[slab] = jnp.concatenate([kept[slab, :, :block], kept[slab, :, block:]], 0).T

            @pl.when(slab < slabs - 1)
            def _():
                pick(kept[slab, :, :block], kept[slab, :, block:], slab + 1)

        @pl.when(c == chunks - 1)
        def _():
            slab = slabs - 1
            near = kept[slab, :, :block]
            upper = jnp.where(local_row < lane, near, jnp.where(local_row == lane, 0.5 * near, 0.0))
            pick(upper, jnp.where(local_row > lane, near, 0.0), 0)
            far = kept[slab, :, block:]
            holds = local_row - lane <= bound_me
            pick(jnp.where(holds, far, 0.0), jnp.where(holds, 0.0, far), slabs)

    def reflect(c):
        for g in range(group):
            slab = c * group + g
            for sub in range(q):
                mirror(slab + 1, sub, slab, slab).start()

        @pl.when(c == chunks - 1)
        def _():
            slab = slabs - 1
            for sub in range(q):

                @pl.when(sub != sub_me)
                def _():
                    mirror(0, sub, slab, slabs).start()

                @pl.when(sub == sub_me)
                def _():
                    mirrored[slabs * q + sub] = turned[slab, sub * own : (sub + 1) * own]

    def late_grams(t, part_of):
        if not inside:
            return
        count = blocks // 4

        @pl.when(t < 3)
        def _():
            begin = (2 * (t - 1) + part_of) * count
            lax.fori_loop(begin, begin + count, compute_late, 0)

        @pl.when(t == 3)
        def _():
            begin = blocks // 2 - late_lag // 2 + part_of * (late_lag // 4)
            for w in range(begin, begin + late_lag // 4):
                join(w, 1, 1)

    def late_sends(t):
        if not inside:
            return

        @pl.when((t >= 3) & (t - 3 < per_pass - 1))
        def _():
            send_later(per_pass + t - 2)

    def body():
        out = []

        def add(at, lowest, action):
            out.append((at - int(at), int(at), lowest, action))

        for s in range(2, nbits):
            at = OFFSETS[0] if s == 2 else s - 2 + (OFFSETS[2] if s == nbits - 1 else OFFSETS[1])
            count = 1 << (nbits - 1 - s)
            for i in range(count):
                v = 2 * count - 1 - i
                add(at + SPREAD * i / count, 1 if s == 2 else 0, functools.partial(item, v, s))
        add(nbits + FINISH_AT, 0, finish)
        add(nbits + FINISH_AT + REFLECT_AFTER, 0, reflect)
        for part_of in range(2):
            out.append((GRAMS_AT[part_of], None, 0, functools.partial(lambda which, t: late_grams(t, which), part_of)))
        out.append((GRAMS_AT[2], None, 0, late_sends))
        return sorted(out, key=lambda entry: entry[0])

    turn_body = body()
    last = max(delay for _, delay, _, _ in turn_body if delay is not None)

    def step(t, _):
        for _, delay, lowest, action in turn_body:
            if delay is None:
                action(t)
                continue
            c = t - delay

            @pl.when((c >= lowest) & (c < chunks))
            def _():
                action(c)

        return 0

    lax.fori_loop(1, chunks + last, step, 0)

    sums = 2.0 * tally[...]
    sum_real = jnp.where(paired > 0, sums, 0.0)
    sum_imag = jnp.where(paired > 0, 0.0, sums)
    phase_real = jnp.where(turn == 0, 1.0, jnp.where(turn == 2, -1.0, 0.0))
    phase_imag = jnp.where(turn == 1, 1.0, jnp.where(turn == 3, -1.0, 0.0))
    total = jnp.concatenate(
        [phase_real * sum_real - phase_imag * sum_imag, phase_real * sum_imag + phase_imag * sum_real], 0
    )
    outbox[...] = total
    inbox[me] = total

    def share(d, to):
        return pltpu.make_async_remote_copy(
            src_ref=outbox,
            dst_ref=inbox.at[to],
            send_sem=esend.at[d],
            recv_sem=erecv.at[to],
            device_id=coords((me + d) % n, sizes),
            device_id_type=MESH,
        )

    def share_out(d, _):
        share(d, me).start()
        return 0

    lax.fori_loop(1, n, share_out, 0)

    for k in range(1, slabs + 1):
        for sub in range(q):
            slot = (k - 1) * q + sub
            mirror_from(k, sub, k - 1).wait()
            mirrored[slot] = came[slot]
    for sub in range(q):

        @pl.when(sub != sub_me)
        def _():
            mirror_from(0, sub, slabs).wait()
            mirrored[slabs * q + sub] = came[slabs * q + sub]

    def drain(ident, _):
        pltpu.make_async_remote_copy(
            src_ref=part.at[0],
            dst_ref=land.at[ident],
            send_sem=send_sem.at[ident],
            recv_sem=recv_sem.at[0],
            device_id=coords(partner[0], sizes),
            device_id_type=MESH,
        ).wait_send()
        return 0

    lax.fori_loop(1, n, drain, 0)

    def share_in(d, _):
        share(d, (me + d) % n).wait()
        return 0

    lax.fori_loop(1, n, share_in, 0)

    total = inbox[0]
    for j in range(1, n):
        total = total + inbox[j]
    expect[...] = total


def finish_kernel(sizes, kept, mirrored, expected, real, imag, expect):
    n = sizes[0] * sizes[1] * sizes[2]
    own, order = real.shape
    block = max(own, LANES)
    q = block // own
    blocks = order // block
    slabs = kept.shape[0]
    me = flat_index(sizes)
    mine = me // q
    sub_me = me % q

    def columns(k):
        return pl.ds(pl.multiple_of(((mine + k + blocks) % blocks) * block, block), block)

    def turned(slot, side):
        return jnp.concatenate([mirrored[slot * q + sub][:, side * own : (side + 1) * own] for sub in range(q)], 1)

    for k in range(1, slabs):
        real[:, columns(k)] = kept[k - 1, :, :block]
        imag[:, columns(k)] = kept[k - 1, :, block:]
        real[:, columns(-k)] = turned(k - 1, 0)
        imag[:, columns(-k)] = -turned(k - 1, 1)
    row = sub_me * own + lax.broadcasted_iota(jnp.int32, (own, block), 0)
    lane = lax.broadcasted_iota(jnp.int32, (own, block), 1)
    near, other = kept[slabs - 1, :, :block], turned(slabs, 0)
    real[:, columns(0)] = jnp.where(row <= lane, near, other)
    imag[:, columns(0)] = jnp.where(row > lane, near, jnp.where(row < lane, -other, 0.0))
    far, other = kept[slabs - 1, :, block:], turned(slabs - 1, 1)
    holds = row - lane <= jnp.where(mine < blocks // 2, 0, -1)
    real[:, columns(slabs)] = jnp.where(holds, far, other)
    imag[:, columns(slabs)] = jnp.where(holds, -other, far)
    expect[...] = expected[...]


def on_device(sizes, amplitudes, pauli_x, pauli_z, pauli_phase):
    n = sizes[0] * sizes[1] * sizes[2]
    _, depth, order = amplitudes.shape
    own = order // n
    block = max(own, LANES)
    q = block // own
    blocks = order // block
    slabs = blocks // 2
    group = min(slabs, max(1, LANES // (2 * own)))
    chunks = slabs // group
    width = (slabs + 1) * block
    slots = (slabs + 1) * q
    vmem = pl.BlockSpec(memory_space=pltpu.VMEM)
    terms = pauli_x.shape[0]
    kept, mirrored, expect = pl.pallas_call(
        functools.partial(gram_kernel, sizes, float(depth * n), min(EARLY, chunks // 2)),
        out_shape=(
            jax.ShapeDtypeStruct((slabs, own, 2 * block), jnp.float32),
            jax.ShapeDtypeStruct((slots, own, 2 * own), jnp.float32),
            jax.ShapeDtypeStruct((2, terms), jnp.float32),
        ),
        in_specs=[pl.BlockSpec(memory_space=pltpu.HBM)] * 4,
        out_specs=(vmem,) * 3,
        scratch_shapes=[
            pltpu.VMEM((2 * depth, order + width - block), jnp.bfloat16),
            *[pltpu.VMEM((1, terms), jnp.int32)] * 3,
            pltpu.VMEM((n, slabs, own, 2 * block), jnp.float32),
            pltpu.VMEM((n, slabs, own, 2 * block), jnp.float32),
            pltpu.VMEM((slabs, block, 2 * own), jnp.float32),
            pltpu.VMEM((slots, own, 2 * own), jnp.float32),
            pltpu.VMEM((6 * own, terms), jnp.bfloat16),
            pltpu.VMEM((1, terms), jnp.float32),
            pltpu.VMEM((2, terms), jnp.float32),
            pltpu.VMEM((n, 2, terms), jnp.float32),
            pltpu.SemaphoreType.DMA((6,)),
            pltpu.SemaphoreType.DMA((3,)),
            pltpu.SemaphoreType.DMA((n,)),
            pltpu.SemaphoreType.DMA((n * chunks,)),
            pltpu.SemaphoreType.DMA((slots,)),
            pltpu.SemaphoreType.DMA((slots,)),
            pltpu.SemaphoreType.DMA((n,)),
            pltpu.SemaphoreType.DMA((n,)),
        ],
        compiler_params=pltpu.CompilerParams(collective_id=0, has_side_effects=True, vmem_limit_bytes=VMEM_LIMIT),
    )(amplitudes, *[pltpu.with_memory_space_constraint(m[None], pltpu.HBM) for m in (pauli_x, pauli_z, pauli_phase)])
    real, imag, expect = pl.pallas_call(
        functools.partial(finish_kernel, sizes),
        out_shape=(
            jax.ShapeDtypeStruct((own, order), jnp.float32),
            jax.ShapeDtypeStruct((own, order), jnp.float32),
            jax.ShapeDtypeStruct((2, terms), jnp.float32),
        ),
        in_specs=[vmem] * 3,
        out_specs=(vmem,) * 3,
        compiler_params=pltpu.CompilerParams(vmem_limit_bytes=8 << 20),
    )(kept, mirrored, expect)
    return real, imag, expect


def solution(mesh):
    sizes = tuple(mesh.shape[axis] for axis in AXES)
    return jax.shard_map(
        functools.partial(on_device, sizes),
        mesh=mesh,
        in_specs=(P(None, AXES, None), P(), P(), P()),
        out_specs=(P(AXES, None), P(AXES, None), P()),
        check_vma=False,
    )
```

```python
import functools

import jax
import jax.numpy as jnp
from jax import lax
from jax.experimental import pallas as pl
from jax.experimental.pallas import tpu as pltpu
from jax.sharding import PartitionSpec as P

AXES = ("gx", "gy", "gz")
LANES = 128
EARLY = 2
OFFSETS = (0.0, 0.12, 0.02)
SPREAD = 0.4
FINISH_AT = 0.124
REFLECT_AFTER = 1.0
GRAMS_AT = (0.28, 0.35, 0.5)
VMEM_LIMIT = 52 << 20
MESH = pl.DeviceIdType.MESH


def log2(value):
    return value.bit_length() - 1


def flat_index(sizes):
    return (lax.axis_index("gx") * sizes[1] + lax.axis_index("gy")) * sizes[2] + lax.axis_index("gz")


def coords(flat, sizes):
    return (flat // (sizes[1] * sizes[2]), (flat // sizes[2]) % sizes[1], flat % sizes[2])


def flip(bit, by):
    return bit + by - 2 * bit * by


def stage_order(sizes):
    zs = log2(sizes[2])
    ys = log2(sizes[1])
    xs = log2(sizes[0])
    rest_x = [zs + ys + t for t in range(xs - 1, 0, -1)]
    rest_y = [zs + t for t in range(ys)]
    rest_z = list(range(zs - 1, -1, -1))
    order = [zs + ys] + rest_x + rest_y[:1] + rest_z + rest_y[1:]
    trade = order.index(rest_z[0]) if rest_x and rest_z else 1
    return order, trade


def parity_sign(masked):
    shift = 16
    while shift >= 1:
        masked = jnp.bitwise_xor(masked, jnp.right_shift(masked, shift))
        shift //= 2
    return (1 - 2 * jnp.bitwise_and(masked, 1)).astype(jnp.float32)


def row_order(sizes, q):
    nbits = log2(sizes[0] * sizes[1] * sizes[2])
    stages, _ = stage_order(sizes)
    lowbits = log2(q)
    return [p for p in stages[2:3] + stages[4:] + stages[1:2] + stages[3:4] if lowbits <= p < nbits]


def early_items(sizes, q, lag, flight):
    nbits = log2(sizes[0] * sizes[1] * sizes[2])
    stages, trade = stage_order(sizes)
    high = row_order(sizes, q)

    def pair_of(v, half):
        by_stage = [(v >> (nbits - 1 - s)) & 1 for s in range(nbits)]
        if half:
            by_stage[1], by_stage[trade] = by_stage[trade], by_stage[1]
        flips = {p: by_stage[s] for s, p in enumerate(stages)}
        w = 0
        for p in high:
            w = 2 * w + 1 - flips[p]
        return w

    out = []
    for v in range((1 << (nbits - 2)) - 1, (1 << (nbits - 3)) - 1, -1):
        waits = []
        for half in range(2):
            waits.append(2 * pair_of(v, half) + 1 + lag)
            waits.append(2 * pair_of(v | (1 << (nbits - 2)), half) + 1 + lag + flight)
        out.append((max(waits), v))
    return sorted(out, key=lambda item: (item[0], -item[1]))


def gram_kernel(
    sizes, total_cols, early, amp, px_in, pz_in, phase_in, kept, mirrored, expect,
    ext, px, pz, phase, part, land, turned, came, spread, tally, outbox, inbox, load_sem, mask_sem, send_sem, recv_sem, msend, mrecv, esend, erecv,
):
    n = sizes[0] * sizes[1] * sizes[2]
    nbits = log2(n)
    depth = amp.shape[1]
    order = amp.shape[2]
    own = order // n
    block = max(own, LANES)
    q = block // own
    blocks = order // block
    width = (blocks // 2 + 1) * block
    slabs = part.shape[1]
    chunks = recv_sem.shape[0] // n
    group = slabs // chunks
    passes = 2
    per_pass = chunks // passes
    part_slabs = slabs // passes
    me = flat_index(sizes)
    bits = [(me // (1 << p)) % 2 for p in range(nbits)]
    stages, trade = stage_order(sizes)
    half = bits[stages[0]]
    lag, late_lag, flight = 4, blocks // 2, 6

    wrap = part_slabs * block

    def loads():
        out = []
        for part_index in range(2):
            rows = pl.ds(part_index * depth, depth)
            out.append(pltpu.make_async_copy(amp.at[part_index], ext.at[rows, pl.ds(0, order)], load_sem.at[2 * part_index]))
            out.append(
                pltpu.make_async_copy(
                    amp.at[part_index, :, pl.ds(0, wrap)],
                    ext.at[rows, pl.ds(order, wrap)],
                    load_sem.at[2 * part_index + 1],
                )
            )
        for part_index in range(2):
            out.append(
                pltpu.make_async_copy(
                    amp.at[part_index, :, pl.ds(wrap, width - block - wrap)],
                    ext.at[pl.ds(part_index * depth, depth), pl.ds(order + wrap, width - block - wrap)],
                    load_sem.at[4 + part_index],
                )
            )
        return out

    def flips_of(v):
        by_stage = [(v >> (nbits - 1 - s)) & 1 for s in range(nbits)]
        flips = [0] * nbits
        for s, p in enumerate(stages):
            flips[p] = by_stage[s]
        flips[stages[1]] = by_stage[1] * (1 - half) + by_stage[trade] * half
        flips[stages[trade]] = by_stage[trade] * (1 - half) + by_stage[1] * half
        return flips

    def place(flips):
        return sum((1 << p) * flip(bits[p], flips[p]) for p in range(nbits))

    def name(flips):
        return sum((1 << p) * flips[p] for p in range(nbits))

    partner = [place(flips_of(1 << (nbits - 1 - s))) for s in range(nbits)]
    barrier = pltpu.get_barrier_semaphore()
    for other in partner:
        pl.semaphore_signal(barrier, inc=1, device_id=coords(other, sizes), device_id_type=MESH)
    for copy in loads():
        copy.start()
    masks = [
        pltpu.make_async_copy(source, target, mask_sem.at[i])
        for i, (source, target) in enumerate(((px_in, px), (pz_in, pz), (phase_in, phase)))
    ]
    for copy in masks:
        copy.start()
    lowbits = log2(q)
    high = row_order(sizes, q)

    def message(where, ident, target, c):
        piece = pl.ds(c * group, group)
        return pltpu.make_async_remote_copy(
            src_ref=part.at[where, piece],
            dst_ref=land.at[ident, piece],
            send_sem=send_sem.at[ident],
            recv_sem=recv_sem.at[ident * chunks + c],
            device_id=coords(target, sizes),
            device_id_type=MESH,
        )

    def across(where, ident, which):
        piece = pl.ds(which * part_slabs, part_slabs)
        return pltpu.make_async_remote_copy(
            src_ref=part.at[where, piece],
            dst_ref=land.at[ident, piece],
            send_sem=send_sem.at[ident],
            recv_sem=recv_sem.at[ident * chunks + which],
            device_id=coords(partner[0], sizes),
            device_id_type=MESH,
        )

    def row_block(u):
        flips = [0] * nbits
        flips[stages[0]] = 1 - u % 2
        for j, p in enumerate(high):
            flips[p] = 1 - (u // (1 << (len(high) - j))) % 2
        return flips

    def with_low(flips, g):
        return [(g >> p) & 1 if p < lowbits else flips[p] for p in range(nbits)]

    def summed(where, names, slab, rows):
        total = part[where, slab, rows, :]
        for ident in names:
            total = total + land[ident, slab, rows, :]
        return total

    def join(w, which, upto):
        for g in range(q):
            flips = with_low(row_block(2 * w + 1), g)
            where, ident = place(flips), name(flips)
            across(where, ident + (1 << stages[0]), which).wait_recv()
            for slab in range(which * part_slabs, (which + 1) * part_slabs):
                for r in range(0, own, 8):
                    rows = pl.ds(r, 8)
                    part[where, slab, rows, :] = summed(where, [ident + (1 << stages[0])], slab, rows)
        for c in range(which * per_pass, which * per_pass + upto):
            send_first(w, c)

    def send_first(w, c):
        for g in range(q):
            flips = with_low(row_block(2 * w + 1), g)
            goes = flips[stages[1]] * (1 - half) + flips[stages[trade]] * half

            @pl.when(goes == 1)
            def _():
                message(place(flips), name(flips), partner[1], c).start()

    def arrive(v, upto, c):
        names = [name(flips_of(v | (1 << (nbits - 1 - t)))) for t in range(1, upto)]
        for ident in names:
            message(0, ident, partner[0], c).wait_recv()
        return names

    def item(v, s, c):
        names = arrive(v, s, c)
        flips = flips_of(v)
        where = place(flips)
        for g in range(group):
            slab = c * group + g
            for r in range(0, own, 8):
                rows = pl.ds(r, 8)
                part[where, slab, rows, :] = summed(where, names, slab, rows)
        message(where, name(flips), partner[s], c).start()

    terms = px.shape[1]
    mine = me // q
    sub_me = me % q
    base = me * own

    for copy in loads()[:4]:
        copy.wait()

    row_in = lax.broadcasted_iota(jnp.int32, (block, block), 0)
    lane_in = lax.broadcasted_iota(jnp.int32, (block, block), 1)
    seconds = early_items(sizes, q, lag, flight)

    def gram(u, which):
        flips = row_block(u)
        first = sum((1 << p) * flip(bits[p], flips[p]) for p in range(lowbits, nbits))
        start = pl.multiple_of(first * own, block)
        lhs = ext[:, pl.ds(start, block)]
        crossed = jnp.concatenate([lhs[depth:], -lhs[:depth]], 0)
        both = jnp.concatenate([lhs, crossed], 1)

        def product(k, count):
            rhs = ext[:, pl.ds(pl.multiple_of(start + k * block, block), count * block)]
            return lax.dot_general(both, rhs, (((0,), (0,)), ((), ())), preferred_element_type=jnp.float32)

        low = which * part_slabs
        rows = product(low + 1, part_slabs)
        closing = which == passes - 1
        plain = part_slabs - 1 if closing else part_slabs
        if closing:
            here = product(0, 1)
            far_cols = slice(plain * block, (plain + 1) * block)
            bound = jnp.where(first // q < blocks // 2, 0, -1)
            near = jnp.where(row_in - lane_in <= 0, here[:block], here[block:])
            far = jnp.where(row_in - lane_in <= bound, rows[:block, far_cols], rows[block:, far_cols])
        for sub in range(q):
            at = slice(sub * own, (sub + 1) * own)
            more = slice(block + sub * own, block + (sub + 1) * own)
            for k in range(plain):
                cols = slice(k * block, (k + 1) * block)
                part[first + sub, low + k, :, 0:block] = rows[at, cols]
                part[first + sub, low + k, :, block : 2 * block] = rows[more, cols]
            if closing:
                part[first + sub, slabs - 1, :, 0:block] = near[at]
                part[first + sub, slabs - 1, :, block : 2 * block] = far[at]

    def hand_over(u, which):
        for g in range(q):
            flips = with_low(row_block(u), g)
            across(place(flips), name(flips), which).start()

    def compute(u, _):
        @pl.when(u == 1)
        def _():
            pl.semaphore_wait(barrier, nbits)

        @pl.when(u % 2 == 1)
        def _():
            hand_over(u - 1, 0)

        @pl.when((u % 2 == 1) & (u >= 1 + lag))
        def _():
            join((u - lag) // 2, 0, early)

        for at in sorted({at for at, _ in seconds if at < blocks}):

            @pl.when(u == at)
            def _():
                for when, v in seconds:
                    if when == at:
                        item(v, 2, 0)

        gram(u, 0)
        return 0

    def compute_late(u, _):
        @pl.when(u % 2 == 1)
        def _():
            hand_over(u - 1, 1)

        @pl.when((u % 2 == 1) & (u >= 1 + late_lag))
        def _():
            join((u - late_lag) // 2, 1, 1)

        gram(u, 1)
        return 0

    def send_later(c):
        for w in range(blocks // 2):
            send_first(w, c)

    lax.fori_loop(0, blocks, compute, 0)
    for copy in loads()[4:]:
        copy.wait()

    for w in range(max(blocks // 2 - lag // 2, 0), blocks // 2):
        join(w, 0, early)
    for at, v in seconds:
        if at >= blocks:
            item(v, 2, 0)
    for c in range(early, per_pass):
        send_later(c)

    inside = per_pass >= 4
    if not inside:
        lax.fori_loop(0, blocks, compute_late, 0)
        for w in range(max(blocks // 2 - late_lag // 2, 0), blocks // 2):
            join(w, 1, per_pass)

    for copy in masks:
        copy.wait()
    turn = phase[...]
    paired = parity_sign(jnp.bitwise_and(px[...], pz[...]))
    wanted = jnp.bitwise_xor(px[...], base)
    lane_terms = lax.broadcasted_iota(jnp.int32, (block, terms), 0)
    row = lax.broadcasted_iota(jnp.int32, (own, block), 0)
    lane = lax.broadcasted_iota(jnp.int32, (own, block), 1)
    ids = base + lax.broadcasted_iota(jnp.int32, (own, terms), 0)
    signs = parity_sign(jnp.bitwise_and(ids, pz[...]))
    signs_real = jnp.where(paired > 0, signs, 0.0)
    signs_imag = jnp.where(paired > 0, 0.0, signs)
    spread[...] = jnp.concatenate([signs_real] * 3 + [signs_imag] * 3, 0).astype(jnp.bfloat16)
    tally[...] = jnp.zeros_like(tally)

    def swapped_rows(values):
        for p in range(log2(own)):
            step = 1 << p
            swapped = jnp.where(
                jnp.bitwise_and(lane, step) != 0,
                pltpu.roll(values, step, 1),
                pltpu.roll(values, block - step, 1),
            )
            values = jnp.where(jnp.bitwise_and(row, step) != 0, swapped, values)
        return values

    def in_three(values):
        high_part = values.astype(jnp.bfloat16)
        rest = values - high_part.astype(jnp.float32)
        middle = rest.astype(jnp.bfloat16)
        low = (rest - middle.astype(jnp.float32)).astype(jnp.bfloat16)
        return [high_part, middle, low]

    def pick(real_values, imag_values, k):
        stacked = jnp.concatenate(in_three(swapped_rows(real_values)) + in_three(swapped_rows(imag_values)), 0)
        sums = lax.dot_general(stacked, spread[...], (((0,), (0,)), ((), ())), preferred_element_type=jnp.float32)
        chosen = jnp.where(lane_terms + ((mine + k) % blocks) * block == wanted, sums, 0.0)
        tally[...] = tally[...] + jnp.sum(chosen, axis=0, keepdims=True)

    def mirror(k, sub, source, slot):
        return pltpu.make_async_remote_copy(
            src_ref=turned.at[source, pl.ds(sub * own, own)],
            dst_ref=came.at[slot * q + sub_me],
            send_sem=msend.at[slot * q + sub],
            recv_sem=mrecv.at[slot * q + sub_me],
            device_id=coords(((mine + k) % blocks) * q + sub, sizes),
            device_id_type=MESH,
        )

    def mirror_from(k, sub, slot):
        return pltpu.make_async_remote_copy(
            src_ref=turned.at[0, pl.ds(sub * own, own)],
            dst_ref=came.at[slot * q + sub],
            send_sem=msend.at[slot * q + sub],
            recv_sem=mrecv.at[slot * q + sub],
            device_id=coords(((mine + k) % blocks) * q + sub, sizes),
            device_id_type=MESH,
        )

    local_row = sub_me * own + row
    bound_me = jnp.where(mine < blocks // 2, 0, -1)

    def finish(c):
        names = arrive(0, nbits, c)
        for g in range(group):
            slab = c * group + g
            for r in range(0, own, 8):
                rows = pl.ds(r, 8)
                kept[slab, rows, :] = summed(me, names, slab, rows) / total_cols
            turned[slab] = jnp.concatenate([kept[slab, :, :block], kept[slab, :, block:]], 0).T

            @pl.when(slab < slabs - 1)
            def _():
                pick(kept[slab, :, :block], kept[slab, :, block:], slab + 1)

        @pl.when(c == chunks - 1)
        def _():
            slab = slabs - 1
            near = kept[slab, :, :block]
            upper = jnp.where(local_row < lane, near, jnp.where(local_row == lane, 0.5 * near, 0.0))
            pick(upper, jnp.where(local_row > lane, near, 0.0), 0)
            far = kept[slab, :, block:]
            holds = local_row - lane <= bound_me
            pick(jnp.where(holds, far, 0.0), jnp.where(holds, 0.0, far), slabs)

    def reflect(c):
        for g in range(group):
            slab = c * group + g
            for sub in range(q):
                mirror(slab + 1, sub, slab, slab).start()

        @pl.when(c == chunks - 1)
        def _():
            slab = slabs - 1
            for sub in range(q):

                @pl.when(sub != sub_me)
                def _():
                    mirror(0, sub, slab, slabs).start()

                @pl.when(sub == sub_me)
                def _():
                    mirrored[slabs * q + sub] = turned[slab, sub * own : (sub + 1) * own]

    def late_grams(t, part_of):
        if not inside:
            return
        count = blocks // 4

        @pl.when(t < 3)
        def _():
            begin = (2 * (t - 1) + part_of) * count
            lax.fori_loop(begin, begin + count, compute_late, 0)

        @pl.when(t == 3)
        def _():
            begin = blocks // 2 - late_lag // 2 + part_of * (late_lag // 4)
            for w in range(begin, begin + late_lag // 4):
                join(w, 1, 1)

    def late_sends(t):
        if not inside:
            return

        @pl.when((t >= 3) & (t - 3 < per_pass - 1))
        def _():
            send_later(per_pass + t - 2)

    def body():
        out = []

        def add(at, lowest, action):
            out.append((at - int(at), int(at), lowest, action))

        for s in range(2, nbits):
            at = OFFSETS[0] if s == 2 else s - 2 + (OFFSETS[2] if s == nbits - 1 else OFFSETS[1])
            count = 1 << (nbits - 1 - s)
            for i in range(count):
                v = 2 * count - 1 - i
                add(at + SPREAD * i / count, 1 if s == 2 else 0, functools.partial(item, v, s))
        add(nbits + FINISH_AT, 0, finish)
        add(nbits + FINISH_AT + REFLECT_AFTER, 0, reflect)
        for part_of in range(2):
            out.append((GRAMS_AT[part_of], None, 0, functools.partial(lambda which, t: late_grams(t, which), part_of)))
        out.append((GRAMS_AT[2], None, 0, late_sends))
        return sorted(out, key=lambda entry: entry[0])

    turn_body = body()
    last = max(delay for _, delay, _, _ in turn_body if delay is not None)

    def step(t, _):
        for _, delay, lowest, action in turn_body:
            if delay is None:
                action(t)
                continue
            c = t - delay

            @pl.when((c >= lowest) & (c < chunks))
            def _():
                action(c)

        return 0

    lax.fori_loop(1, chunks + last, step, 0)

    sums = 2.0 * tally[...]
    sum_real = jnp.where(paired > 0, sums, 0.0)
    sum_imag = jnp.where(paired > 0, 0.0, sums)
    phase_real = jnp.where(turn == 0, 1.0, jnp.where(turn == 2, -1.0, 0.0))
    phase_imag = jnp.where(turn == 1, 1.0, jnp.where(turn == 3, -1.0, 0.0))
    total = jnp.concatenate(
        [phase_real * sum_real - phase_imag * sum_imag, phase_real * sum_imag + phase_imag * sum_real], 0
    )
    outbox[...] = total
    inbox[me] = total

    def share(d, to):
        return pltpu.make_async_remote_copy(
            src_ref=outbox,
            dst_ref=inbox.at[to],
            send_sem=esend.at[d],
            recv_sem=erecv.at[to],
            device_id=coords((me + d) % n, sizes),
            device_id_type=MESH,
        )

    def share_out(d, _):
        share(d, me).start()
        return 0

    lax.fori_loop(1, n, share_out, 0)

    for k in range(1, slabs + 1):
        for sub in range(q):
            slot = (k - 1) * q + sub
            mirror_from(k, sub, k - 1).wait()
            mirrored[slot] = came[slot]
    for sub in range(q):

        @pl.when(sub != sub_me)
        def _():
            mirror_from(0, sub, slabs).wait()
            mirrored[slabs * q + sub] = came[slabs * q + sub]

    def drain(ident, _):
        pltpu.make_async_remote_copy(
            src_ref=part.at[0],
            dst_ref=land.at[ident],
            send_sem=send_sem.at[ident],
            recv_sem=recv_sem.at[0],
            device_id=coords(partner[0], sizes),
            device_id_type=MESH,
        ).wait_send()
        return 0

    lax.fori_loop(1, n, drain, 0)

    def share_in(d, _):
        share(d, (me + d) % n).wait()
        return 0

    lax.fori_loop(1, n, share_in, 0)

    total = inbox[0]
    for j in range(1, n):
        total = total + inbox[j]
    expect[...] = total


def finish_kernel(sizes, kept, mirrored, expected, real, imag, expect):
    n = sizes[0] * sizes[1] * sizes[2]
    own, order = real.shape
    block = max(own, LANES)
    q = block // own
    blocks = order // block
    slabs = kept.shape[0]
    me = flat_index(sizes)
    mine = me // q
    sub_me = me % q

    def columns(k):
        return pl.ds(pl.multiple_of(((mine + k + blocks) % blocks) * block, block), block)

    def turned(slot, side):
        return jnp.concatenate([mirrored[slot * q + sub][:, side * own : (side + 1) * own] for sub in range(q)], 1)

    for k in range(1, slabs):
        real[:, columns(k)] = kept[k - 1, :, :block]
        imag[:, columns(k)] = kept[k - 1, :, block:]
        real[:, columns(-k)] = turned(k - 1, 0)
        imag[:, columns(-k)] = -turned(k - 1, 1)
    row = sub_me * own + lax.broadcasted_iota(jnp.int32, (own, block), 0)
    lane = lax.broadcasted_iota(jnp.int32, (own, block), 1)
    near, other = kept[slabs - 1, :, :block], turned(slabs, 0)
    real[:, columns(0)] = jnp.where(row <= lane, near, other)
    imag[:, columns(0)] = jnp.where(row > lane, near, jnp.where(row < lane, -other, 0.0))
    far, other = kept[slabs - 1, :, block:], turned(slabs - 1, 1)
    holds = row - lane <= jnp.where(mine < blocks // 2, 0, -1)
    real[:, columns(slabs)] = jnp.where(holds, far, other)
    imag[:, columns(slabs)] = jnp.where(holds, -other, far)
    expect[...] = expected[...]


def on_device(sizes, amplitudes, pauli_x, pauli_z, pauli_phase):
    n = sizes[0] * sizes[1] * sizes[2]
    _, depth, order = amplitudes.shape
    own = order // n
    block = max(own, LANES)
    q = block // own
    blocks = order // block
    slabs = blocks // 2
    group = min(slabs, max(1, LANES // (2 * own)))
    chunks = slabs // group
    width = (slabs + 1) * block
    slots = (slabs + 1) * q
    vmem = pl.BlockSpec(memory_space=pltpu.VMEM)
    terms = pauli_x.shape[0]
    kept, mirrored, expect = pl.pallas_call(
        functools.partial(gram_kernel, sizes, float(depth * n), min(EARLY, chunks // 2)),
        out_shape=(
            jax.ShapeDtypeStruct((slabs, own, 2 * block), jnp.float32),
            jax.ShapeDtypeStruct((slots, own, 2 * own), jnp.float32),
            jax.ShapeDtypeStruct((2, terms), jnp.float32),
        ),
        in_specs=[pl.BlockSpec(memory_space=pltpu.HBM)] * 4,
        out_specs=(vmem,) * 3,
        scratch_shapes=[
            pltpu.VMEM((2 * depth, order + width - block), jnp.bfloat16),
            *[pltpu.VMEM((1, terms), jnp.int32)] * 3,
            pltpu.VMEM((n, slabs, own, 2 * block), jnp.float32),
            pltpu.VMEM((n, slabs, own, 2 * block), jnp.float32),
            pltpu.VMEM((slabs, block, 2 * own), jnp.float32),
            pltpu.VMEM((slots, own, 2 * own), jnp.float32),
            pltpu.VMEM((6 * own, terms), jnp.bfloat16),
            pltpu.VMEM((1, terms), jnp.float32),
            pltpu.VMEM((2, terms), jnp.float32),
            pltpu.VMEM((n, 2, terms), jnp.float32),
            pltpu.SemaphoreType.DMA((6,)),
            pltpu.SemaphoreType.DMA((3,)),
            pltpu.SemaphoreType.DMA((n,)),
            pltpu.SemaphoreType.DMA((n * chunks,)),
            pltpu.SemaphoreType.DMA((slots,)),
            pltpu.SemaphoreType.DMA((slots,)),
            pltpu.SemaphoreType.DMA((n,)),
            pltpu.SemaphoreType.DMA((n,)),
        ],
        compiler_params=pltpu.CompilerParams(collective_id=0, has_side_effects=True, vmem_limit_bytes=VMEM_LIMIT),
    )(amplitudes, *[pltpu.with_memory_space_constraint(m[None], pltpu.HBM) for m in (pauli_x, pauli_z, pauli_phase)])
    real, imag, expect = pl.pallas_call(
        functools.partial(finish_kernel, sizes),
        out_shape=(
            jax.ShapeDtypeStruct((own, order), jnp.float32),
            jax.ShapeDtypeStruct((own, order), jnp.float32),
            jax.ShapeDtypeStruct((2, terms), jnp.float32),
        ),
        in_specs=[vmem] * 3,
        out_specs=(vmem,) * 3,
        compiler_params=pltpu.CompilerParams(vmem_limit_bytes=8 << 20),
    )(kept, mirrored, expect)
    return real, imag, expect


def solution(mesh):
    sizes = tuple(mesh.shape[axis] for axis in AXES)
    return jax.shard_map(
        functools.partial(on_device, sizes),
        mesh=mesh,
        in_specs=(P(None, AXES, None), P(), P(), P()),
        out_specs=(P(AXES, None), P(AXES, None), P()),
        check_vma=False,
    )
```
